256 devices in a mesh: gz: 32 (over x, z), gy: 8 (over y, core).
Axes of the slice: x: 4, y: 4, z: 8, core: 2. Of those that a mesh axis runs over, the one named last changes fastest.
Arguments:
- fields: float32 [2, 256, 256, 128], P(None, 'gz', 'gy'), may hold values from -7 to 8
- residual: float32 [2, 256, 256, 128], P(None, 'gz', 'gy'), may hold values from -14 to 14
- past_fields: float32 [20, 2, 256, 256, 128], P(None, None, 'gz', 'gy'), may hold values from -7 to 8
- past_residuals: float32 [20, 2, 256, 256, 128], P(None, None, 'gz', 'gy'), may hold values from -14 to 14
Outputs:
- new_fields: float32 [2, 256, 256, 128], P(None, 'gz', 'gy')
- summary: float32 [3], replicated
The draws below stay inside these ranges and needn't reach their ends.
All inputs are finite; a program needn't handle non-finite values.
Results may differ from the reference program's by a relative error of at most 0.0003.
Values sent between devices are 32-bit elements; how exact they have to be, the bound alone decides.
No kernel may reach another device: no remote copies, remote signals or barrier semaphores. Data moves between devices by JAX's collectives and lax.ppermute only.
A program may use at most 64 MiB of HBM per device.

```python
import math
import jax
import jax.numpy as jnp
from jax import lax

HIST = 20
NZ = 256
NY = 256
NX = 128


TWO_PI = 2.0 * math.pi


def low_modes(key, count):
    amplitude = jax.random.uniform(jax.random.fold_in(key, 1), (count, 4), jnp.float32, -1.0, 1.0)
    phase = jax.random.uniform(jax.random.fold_in(key, 2), (count, 4), jnp.float32, 0.0, TWO_PI)
    height = (lax.iota(jnp.int32, NZ).astype(jnp.float32) / NZ)[None, :, None]
    width = (lax.iota(jnp.int32, NY).astype(jnp.float32) / NY)[None, None, :]
    total = amplitude[:, 0, None, None] * jnp.sin(TWO_PI * height + phase[:, 0, None, None])
    total = total + amplitude[:, 1, None, None] * jnp.sin(TWO_PI * width + phase[:, 1, None, None])
    total = total + amplitude[:, 2, None, None] * jnp.sin(TWO_PI * (height + width) + phase[:, 2, None, None])
    total = total + amplitude[:, 3, None, None] * jnp.sin(TWO_PI * (2.0 * height - width) + phase[:, 3, None, None])
    return total


def high_modes(key):
    phase = jax.random.uniform(jax.random.fold_in(key, 1), (5,), jnp.float32, 0.0, TWO_PI)
    height = lax.iota(jnp.int32, NZ).astype(jnp.float32) / NZ
    width = lax.iota(jnp.int32, NY).astype(jnp.float32) / NY
    line = lax.iota(jnp.int32, NX).astype(jnp.float32) / NX
    third_z = jnp.sin(TWO_PI * 3.0 * height + phase[0])[:, None, None] * jnp.cos(TWO_PI * line + phase[1])[None, None, :]
    fourth_y = jnp.sin(TWO_PI * 4.0 * width + phase[2])[None, :, None] * jnp.cos(TWO_PI * 2.0 * line + phase[3])[None, None, :]
    slanted = jnp.sin(TWO_PI * (5.0 * height[:, None] + 3.0 * width[None, :]) + phase[4])[:, :, None]
    pattern = 1.5 * third_z + 1.0 * fourth_y + 0.8 * slanted
    species_sign = jnp.array([1.0, -0.8], jnp.float32)
    return species_sign[:, None, None, None] * pattern[None, :, :, :]


def current_residual(key):
    source = jax.random.fold_in(key, 101)
    spread = jnp.exp(jax.random.uniform(jax.random.fold_in(source, 1), (NZ,), jnp.float32, -0.7, 0.7))
    rough = jnp.clip(jax.random.normal(jax.random.fold_in(source, 2), (2, NZ, NY, NX), jnp.float32), -2.5, 2.5)
    offset = jax.random.uniform(jax.random.fold_in(source, 3), (NZ, NY), jnp.float32, -0.8, 0.8)
    broad = 1.2 * low_modes(jax.random.fold_in(source, 4), 1)[0]
    sharp = high_modes(jax.random.fold_in(source, 5))
    total = rough * spread[None, :, None, None] + (offset + broad)[None, :, :, None] + sharp
    return jnp.clip(total, -14.0, 14.0)


def draw_residual(key, part):
    return current_residual(key)


def draw_past_residuals(key, part):
    current = current_residual(key)
    source = jax.random.fold_in(key, 202)
    decay = jax.random.uniform(jax.random.fold_in(source, 1), (HIST,), jnp.float32, 0.3, 0.95)
    weight = jnp.exp(jax.random.uniform(jax.random.fold_in(source, 2), (HIST,), jnp.float32, math.log(0.4), 0.0))
    phase = jax.random.uniform(jax.random.fold_in(source, 3), (HIST, 2), jnp.float32, 0.0, TWO_PI)
    bumps = jax.random.uniform(jax.random.fold_in(source, 4), (HIST, NZ), jnp.float32, -0.15, 0.15)
    broad = low_modes(jax.random.fold_in(source, 5), HIST)
    height = lax.iota(jnp.int32, NZ).astype(jnp.float32) / NZ
    width = lax.iota(jnp.int32, NY).astype(jnp.float32) / NY
    shared = jnp.zeros((), jnp.float32)
    own_share = 1.0
    shared_share = 0.0

    def one_iterate(index):
        tilt = 0.6 * jnp.sin(TWO_PI * height + phase[index, 0])[:, None] + 0.3 * jnp.sin(TWO_PI * width + phase[index, 1])[None, :] + bumps[index][:, None]
        envelope = jnp.exp(tilt)
        rough = jnp.clip(jax.random.normal(jax.random.fold_in(source, 1000 + index), (2, NZ, NY, NX), jnp.float32), -2.5, 2.5)
        sharp = 0.6 * high_modes(jax.random.fold_in(source, 2000 + index))
        noise = (own_share * rough + shared_share * shared + 0.5 * broad[index][None, :, :, None]) * envelope[None, :, :, None] + sharp
        return jnp.clip(decay[index] * current + weight[index] * noise, -14.0, 14.0)
    return lax.map(one_iterate, lax.iota(jnp.int32, HIST))


def species_field(key):
    spread = 1.5
    rough = jnp.clip(jax.random.normal(key, (2, NZ, NY, NX), jnp.float32), -3.0, 3.0)
    level = jnp.array([2.0, -1.0], jnp.float32)
    return spread * rough + level[:, None, None, None]


def draw_fields(key, part):
    return species_field(jax.random.fold_in(key, 303))


def draw_past_fields(key, part):
    source = jax.random.fold_in(key, 404)

    def one_iterate(index):
        return species_field(jax.random.fold_in(source, index))
    return lax.map(one_iterate, lax.iota(jnp.int32, HIST))


def setup_inputs(seed: int = 0) -> dict:
    streams_of = jax.random.split(jax.random.key(seed), 5)
    fields = draw_fields(jax.random.fold_in(streams_of[4], 71), 0)
    residual = draw_residual(jax.random.fold_in(streams_of[4], 71), 0)
    past_fields = draw_past_fields(jax.random.fold_in(streams_of[4], 71), 0)
    past_residuals = draw_past_residuals(jax.random.fold_in(streams_of[4], 71), 0)
    return {"fields": fields, "residual": residual, "past_fields": past_fields, "past_residuals": past_residuals}


CHI_N = 20.0
RIDGE = 0.01
STEP_LOCAL = 0.1
EXACT = lax.Precision.HIGHEST

def kernel_table(length):
    decay_len = length / 4.0
    row_index = lax.iota(jnp.int32, length)[:, None]
    col_index = lax.iota(jnp.int32, length)[None, :]
    lag = jnp.mod(row_index - col_index, length).astype(jnp.float32)
    offsets = lax.iota(jnp.int32, length).astype(jnp.float32)
    normalizer = jnp.sum(jnp.cosh((0.5 * length - offsets) / decay_len))
    return jnp.cosh((0.5 * length - lag) / decay_len) / normalizer

def reference(fields, residual, past_fields, past_residuals):
    history = past_residuals.shape[0]

    def gram_step(plane, carry):
        gram_acc, intersect_acc = carry
        current = lax.dynamic_slice_in_dim(residual, plane, 1, 1).reshape(-1)
        earlier = lax.dynamic_slice_in_dim(past_residuals, plane, 1, 2).reshape(history, -1)
        deltas = current[None, :] - earlier
        gram_acc = gram_acc + jnp.dot(deltas.astype(jnp.float32), deltas.T.astype(jnp.float32), precision=EXACT, preferred_element_type=jnp.float32)
        intersect_acc = intersect_acc + jnp.dot(deltas.astype(jnp.float32), current.astype(jnp.float32), precision=EXACT, preferred_element_type=jnp.float32)
        return (gram_acc, intersect_acc)
    start = (jnp.zeros((history, history), jnp.float32), jnp.zeros((history,), jnp.float32))
    gram_matrix, intersect = lax.fori_loop(0, NZ, gram_step, start)
    diagonal_shift = RIDGE * jnp.trace(gram_matrix) / history + 1.0
    system = gram_matrix + diagonal_shift * jnp.eye(history, dtype=jnp.float32)
    factor = jnp.linalg.cholesky(system)
    forward = lax.linalg.triangular_solve(factor, intersect[:, None], left_side=True, lower=True)
    coeffs = lax.linalg.triangular_solve(factor, forward, left_side=True, lower=True, transpose_a=True)[:, 0]
    remain_weight = 1.0 - jnp.sum(coeffs)
    field_mixed = remain_weight * fields + jnp.dot(coeffs.astype(jnp.float32), past_fields.reshape(history, -1).astype(jnp.float32), precision=EXACT, preferred_element_type=jnp.float32).reshape(fields.shape)
    residual_mixed = remain_weight * residual + jnp.dot(coeffs.astype(jnp.float32), past_residuals.reshape(history, -1).astype(jnp.float32), precision=EXACT, preferred_element_type=jnp.float32).reshape(residual.shape)
    kernel_z = kernel_table(NZ)
    kernel_y = kernel_table(NY)
    smoothed = jnp.einsum('ab,sbyx->sayx', kernel_z, residual_mixed, precision=EXACT)
    smoothed = jnp.einsum('ab,szbx->szax', kernel_y, smoothed, precision=EXACT)
    new_fields = field_mixed + STEP_LOCAL * residual_mixed + smoothed
    split_field = new_fields[0] - new_fields[1]
    sum_field = new_fields[0] + new_fields[1]
    energy = jnp.mean(split_field * split_field / (4.0 * CHI_N) - 0.5 * sum_field)
    relative = jnp.sqrt(jnp.sum(residual * residual) / (jnp.sum(fields * fields) + 1.0))
    largest = jnp.max(jnp.abs(residual_mixed))
    summary = jnp.stack([energy, relative, largest])
    return (new_fields, summary)
```

```python
import functools
import math

import jax
import jax.numpy as jnp
from jax import lax
from jax.experimental import pallas as pl
from jax.experimental.pallas import tpu as pltpu
from jax.sharding import PartitionSpec as P

CHI_N = 20.0
RIDGE = 0.01
STEP_LOCAL = 0.1
EXACT = lax.Precision.HIGHEST
HIST = 20
BANDS = HIST + 2
LINES = 512
CHUNK = 64
LANES = 128
PLANES = 8
ROWS = 32
F32 = jnp.float32
BF16 = jnp.bfloat16
LENGTH = 256
DECAY = LENGTH / 4.0
TOTAL = sum(math.cosh((0.5 * LENGTH - d) / DECAY) for d in range(LENGTH))
WIDE = math.exp(0.5 * LENGTH / DECAY)
CELLS = 256 * 256 * 128

VMEM = pl.BlockSpec(memory_space=pltpu.VMEM)


def params(mib, **more):
    return pltpu.CompilerParams(vmem_limit_bytes=mib * 1024 * 1024, **more)


def halves(x):
    high = x.astype(BF16)
    return high, (x - high.astype(F32)).astype(BF16)


def product(a, b, contract):
    return lax.dot_general(a, b, (contract, ((), ())), preferred_element_type=F32)


def split_product(a, b, contract):
    a_high, a_low = halves(a)
    b_high, b_low = halves(b)
    return (
        product(a_high, b_high, contract)
        + product(a_high, b_low, contract)
        + product(a_low, b_high, contract)
    )


def iota(shape, dim):
    return lax.broadcasted_iota(jnp.int32, shape, dim)


def ramp(shape, dim, sign):
    return jnp.exp(iota(shape, dim).astype(F32) * (sign / DECAY))


def near_matrix(count):
    lag = jnp.abs(iota((count, count), 0) - iota((count, count), 1)).astype(F32)
    half = (0.5 * LENGTH - lag) / DECAY
    return (jnp.exp(half) + jnp.exp(-half)) * (0.5 / TOTAL)


def near_value(lag):
    return math.cosh((0.5 * LENGTH - lag) / DECAY) / TOTAL


def far_weight(row, col, width):
    gap = (row - col).astype(F32) * (width / DECAY)
    below = jnp.exp(-gap) * (WIDE * 0.5 / TOTAL)
    above = jnp.exp(-gap) * (0.5 / (WIDE * TOTAL))
    return jnp.where(col < row, below, jnp.where(col > row, above, 0.0))


def gram_kernel(res_ref, fld_ref, past_ref, out_ref, acc_ref):
    step = pl.program_id(0)
    pieces = []
    for k in range(CHUNK // 8):
        rows = slice(8 * k, 8 * k + 8)
        res = res_ref[rows, :]
        delta = res[None] - past_ref[:, rows, :]
        pieces.append(
            jnp.concatenate([delta.reshape(HIST * 8, LANES), res, fld_ref[rows, :]], axis=0)
        )
    wide = jnp.concatenate(pieces, axis=1)
    part = split_product(wide, wide, ((1,), (1,)))

    @pl.when(step == 0)
    def _():
        acc_ref[...] = part

    @pl.when(step > 0)
    def _():
        acc_ref[...] += part

    @pl.when(step == LINES // CHUNK - 1)
    def _():
        size = BANDS * 8
        same = (iota((size, size), 0) & 7) == (iota((size, size), 1) & 7)
        total = jnp.where(same, acc_ref[...], 0.0)
        columns = (iota((size, LANES), 0) >> 3 == iota((size, LANES), 1)).astype(F32)
        rows = (iota((24, size), 1) >> 3 == iota((24, size), 0)).astype(F32)
        folded = lax.dot(rows, lax.dot(total, columns, precision=EXACT), precision=EXACT)
        packed = (
            folded[0:8]
            + pltpu.roll(folded[8:16], 32, 1)
            + pltpu.roll(folded[16:24], 64, 1)
        )
        out_ref[...] = jnp.broadcast_to(packed[None], out_ref.shape)


def gram_partial(res, fld, past, copies):
    return pl.pallas_call(
        gram_kernel,
        grid=(LINES // CHUNK,),
        out_shape=jax.ShapeDtypeStruct((copies, 8, LANES), F32),
        in_specs=[
            pl.BlockSpec((CHUNK, LANES), lambda t: (t, 0)),
            pl.BlockSpec((CHUNK, LANES), lambda t: (t, 0)),
            pl.BlockSpec((HIST, CHUNK, LANES), lambda t: (0, t, 0)),
        ],
        out_specs=pl.BlockSpec((copies, 8, LANES), lambda t: (0, 0, 0)),
        scratch_shapes=[pltpu.VMEM((BANDS * 8, BANDS * 8), F32)],
        compiler_params=params(12),
        name="gram",
    )(res, fld, past)


def solve(packed):
    place = iota((24, LANES), 0)

    def column(i):
        parts = [
            jnp.broadcast_to(packed[:, 32 * b + i : 32 * b + i + 1], (8, LANES)) for b in range(3)
        ]
        return jnp.concatenate(parts, axis=0)

    rows = [column(i) for i in range(HIST)]
    right = column(HIST)
    trace = rows[0][0:1]
    for i in range(1, HIST):
        trace = trace + rows[i][i : i + 1]
    shift = (RIDGE / HIST) * trace + 1.0
    rows = [rows[i] + jnp.where(place == i, shift, 0.0) for i in range(HIST)]
    inverse = []
    for k in range(HIST):
        inv = 1.0 / rows[k][k : k + 1]
        inverse.append(inv)
        after = jnp.where(place > k, rows[k] * inv, 0.0)
        for i in range(k + 1, HIST):
            rows[i] = rows[i] - after * rows[i][k : k + 1]
        right = right - after * right[k : k + 1]
    coeffs = [None] * HIST
    for k in reversed(range(HIST)):
        coeffs[k] = right[k : k + 1] * inverse[k]
        right = right - jnp.where(place < k, rows[k] * coeffs[k], 0.0)
    remain = 1.0 - functools.reduce(jnp.add, coeffs)
    return remain, coeffs


def mix_kernel(sums_ref, res_ref, past_ref, mixed_ref, moment_ref, coeff_ref):
    packed = jnp.sum(sums_ref[...], axis=0)
    remain, coeffs = solve(packed)
    for i in range(HIST):
        coeff_ref[i : i + 1, :] = coeffs[i]
    coeff_ref[HIST : HIST + 1, :] = remain
    res_square = packed[4:5, 64 + HIST : 65 + HIST]
    fld_square = packed[5:6, 65 + HIST : 66 + HIST]
    coeff_ref[21:22, :] = jnp.broadcast_to(jnp.sqrt(res_square / (fld_square + 1.0)), (1, LANES))
    spread = [jnp.broadcast_to(c, (ROWS, LANES)) for c in coeffs]
    remain = jnp.broadcast_to(remain, (ROWS, LANES))
    rise = ramp((ROWS, LANES), 0, 1.0)
    fall = ramp((ROWS, LANES), 0, -1.0)
    for plane in range(2 * PLANES):
        rows = slice(ROWS * plane, ROWS * plane + ROWS)
        total = remain * res_ref[rows, :]
        for i in range(HIST):
            total = total + spread[i] * past_ref[i, rows, :]
        mixed_ref[rows, :] = total
        s, z = divmod(plane, PLANES)
        moment_ref[0, s, z : z + 1, :] = jnp.sum(rise * total, axis=0, keepdims=True)
        moment_ref[0, 2 + s, z : z + 1, :] = jnp.sum(fall * total, axis=0, keepdims=True)
    for k in range(1, moment_ref.shape[0]):
        moment_ref[k] = moment_ref[0]


def mix(sums, res, past, copies):
    return pl.pallas_call(
        mix_kernel,
        out_shape=(
            jax.ShapeDtypeStruct((LINES, LANES), F32),
            jax.ShapeDtypeStruct((copies, 4, PLANES, LANES), F32),
            jax.ShapeDtypeStruct((24, LANES), F32),
        ),
        in_specs=[VMEM] * 3,
        out_specs=(VMEM,) * 3,
        compiler_params=params(16),
        name="mix",
    )(sums, res, past)


def local_kernel(coeff_ref, fld_ref, past_ref, mixed_ref, base_ref, moment_ref, near_ref):
    wide = jnp.concatenate(
        [mixed_ref[ROWS * k : ROWS * k + ROWS, :] for k in range(2 * PLANES)], axis=1
    )
    near = split_product(near_matrix(ROWS), wide, ((1,), (0,)))
    for k in range(2 * PLANES):
        near_ref[ROWS * k : ROWS * k + ROWS, :] = near[:, LANES * k : LANES * k + LANES]
    coeffs = [jnp.broadcast_to(coeff_ref[i : i + 1, :], (ROWS, LANES)) for i in range(HIST + 1)]
    peak = jnp.zeros((ROWS, LANES), F32)
    for s in range(2):
        planes = [near_ref[ROWS * k : ROWS * k + ROWS, :] for k in range(PLANES * s, PLANES * s + PLANES)]
        rising = planes[0]
        falling = planes[0]
        for z in range(1, PLANES):
            rising = rising + math.exp(z / DECAY) * planes[z]
            falling = falling + math.exp(-z / DECAY) * planes[z]
        moment_ref[s] = rising
        moment_ref[2 + s] = falling
        for z in range(PLANES):
            rows = slice(ROWS * (PLANES * s + z), ROWS * (PLANES * s + z) + ROWS)
            own = mixed_ref[rows, :]
            peak = jnp.maximum(peak, jnp.abs(own))
            total = STEP_LOCAL * own + coeffs[HIST] * fld_ref[rows, :]
            for i in range(HIST):
                total = total + coeffs[i] * past_ref[i, rows, :]
            for z2 in range(PLANES):
                total = total + near_value(abs(z - z2)) * planes[z2]
            base_ref[rows, :] = total
    moment_ref[4] = peak


def local_part(coeffs, fld, past, mixed):
    return pl.pallas_call(
        local_kernel,
        out_shape=(
            jax.ShapeDtypeStruct((LINES, LANES), F32),
            jax.ShapeDtypeStruct((5, ROWS, LANES), F32),
        ),
        in_specs=[VMEM] * 4,
        out_specs=(VMEM,) * 2,
        scratch_shapes=[pltpu.VMEM((LINES, LANES), F32)],
        compiler_params=params(16),
        name="local_part",
    )(coeffs, fld, past, mixed)


def column_kernel(ends_ref, base_ref, moment_ref, full_ref, send_ref):
    here = lax.axis_index("gy")
    count = ends_ref.shape[0]
    shape = (count, LANES)
    other = iota(shape, 0)
    down = far_weight(jnp.full(shape, here, jnp.int32), other, ROWS)
    up = far_weight(other, jnp.full(shape, here, jnp.int32), ROWS)
    fields = []
    for kind, weight in ((0, down), (2, up)):
        for s in range(2):
            total = weight[0:1] * ends_ref[0, kind + s]
            for q in range(1, count):
                total = total + weight[q : q + 1] * ends_ref[q, kind + s]
            fields.append(total)
    wide = jnp.concatenate(fields, axis=1)
    row = iota((16, PLANES), 0)
    col = iota((16, PLANES), 1)
    lag = (0.5 * LENGTH - jnp.abs(row - col).astype(F32)) / DECAY
    near = (jnp.exp(lag) + jnp.exp(-lag)) * (0.5 / TOTAL)
    rise = jnp.exp(col.astype(F32) / DECAY)
    fall = jnp.exp(col.astype(F32) / -DECAY)
    mixer = jnp.where(row < 8, near, jnp.where(row == 8, rise, fall))
    smooth = lax.dot(mixer, wide, precision=EXACT)

    fall_y = ramp((ROWS, LANES), 0, -1.0)
    rise_y = ramp((ROWS, LANES), 0, 1.0)

    def spread(line, s):
        return (
            fall_y * smooth[line : line + 1, LANES * s : LANES * s + LANES]
            + rise_y * smooth[line : line + 1, LANES * (2 + s) : LANES * (2 + s) + LANES]
        )

    def put(k, value):
        send_ref[pl.ds(k, ROWS, stride=8), :] = value

    for s in range(2):
        put(s, moment_ref[s] + spread(8, s))
        put(2 + s, moment_ref[2 + s] + spread(9, s))
    first = jnp.zeros((ROWS, LANES), F32)
    second = jnp.zeros((ROWS, LANES), F32)
    energy = jnp.zeros((ROWS, LANES), F32)
    for z in range(PLANES):
        pair = []
        for s in range(2):
            rows = slice(ROWS * (PLANES * s + z), ROWS * (PLANES * s + z) + ROWS)
            value = base_ref[rows, :] + spread(z, s)
            full_ref[rows, :] = value
            pair.append(value)
        gap = pair[0] - pair[1]
        first = first + math.exp(-z / DECAY) * gap
        second = second + math.exp(z / DECAY) * gap
        energy = energy + (gap * gap * (1.0 / (4.0 * CHI_N)) - 0.5 * (pair[0] + pair[1]))
    put(4, first)
    put(5, second)
    put(6, energy)
    put(7, moment_ref[4])


def column_part(ends, base, moments, owners):
    return pl.pallas_call(
        column_kernel,
        out_shape=(
            jax.ShapeDtypeStruct((LINES, LANES), F32),
            jax.ShapeDtypeStruct((owners * 8, LANES), F32),
        ),
        in_specs=[VMEM] * 3,
        out_specs=(VMEM,) * 2,
        compiler_params=params(8),
        name="column_part",
    )(ends, base, moments)


def owner_kernel(got_ref, send_ref):
    count = got_ref.shape[0] // 8
    take = lambda k: got_ref[pl.ds(k, count, stride=8), :]
    row = iota((count, count), 0)
    col = iota((count, count), 1)
    rising = jnp.concatenate([take(0), take(1)], axis=1)
    falling = jnp.concatenate([take(2), take(3)], axis=1)
    down = split_product(far_weight(row, col, PLANES), rising, ((1,), (0,)))
    up = split_product(far_weight(col, row, PLANES), falling, ((1,), (0,)))
    down = (down[:, :LANES], down[:, LANES:])
    up = (up[:, :LANES], up[:, LANES:])
    fall_sum = sum(math.exp(-z / DECAY) for z in range(PLANES))
    rise_sum = sum(math.exp(z / DECAY) for z in range(PLANES))
    fall_square = sum(math.exp(-2.0 * z / DECAY) for z in range(PLANES))
    rise_square = sum(math.exp(2.0 * z / DECAY) for z in range(PLANES))
    a = down[0] - down[1]
    b = up[0] - up[1]
    square = (
        a * (2.0 * take(4) + fall_square * a + (2.0 * PLANES) * b)
        + b * (2.0 * take(5) + rise_square * b)
    )
    energy = (
        take(6)
        + square * (1.0 / (4.0 * CHI_N))
        - 0.5 * (fall_sum * (down[0] + down[1]) + rise_sum * (up[0] + up[1]))
    )
    energy = jnp.sum(energy, axis=0, keepdims=True)
    peak = jnp.max(take(7), axis=0, keepdims=True)
    values = (*down, *up, energy, peak, peak, peak)
    for k, value in enumerate(values):
        send_ref[pl.ds(k, count, stride=8), :] = jnp.broadcast_to(value, (count, LANES))


def owner_part(got):
    return pl.pallas_call(
        owner_kernel,
        out_shape=jax.ShapeDtypeStruct(got.shape, F32),
        in_specs=[VMEM],
        out_specs=VMEM,
        compiler_params=params(8),
        name="owner_part",
    )(got)


def tally_kernel(got_ref, out_ref):
    energy = jnp.sum(got_ref[pl.ds(4, ROWS, stride=8), :], axis=0, keepdims=True)
    peak = jnp.max(got_ref[pl.ds(5, ROWS, stride=8), :], axis=0, keepdims=True)
    value = jnp.where(iota((8, LANES), 0) == 0, energy, peak)
    out_ref[...] = jnp.broadcast_to(value[None], out_ref.shape)


def tally(got, copies):
    return pl.pallas_call(
        tally_kernel,
        out_shape=jax.ShapeDtypeStruct((copies, 8, LANES), F32),
        in_specs=[VMEM],
        out_specs=VMEM,
        compiler_params=params(8),
        name="tally",
    )(got)


def finish_kernel(got_ref, full_ref, out_ref):
    down = [got_ref[pl.ds(s, ROWS, stride=8), :] for s in range(2)]
    up = [got_ref[pl.ds(2 + s, ROWS, stride=8), :] for s in range(2)]
    for s in range(2):
        for z in range(PLANES):
            rows = slice(ROWS * (PLANES * s + z), ROWS * (PLANES * s + z) + ROWS)
            out_ref[rows, :] = (
                full_ref[rows, :]
                + math.exp(-z / DECAY) * down[s]
                + math.exp(z / DECAY) * up[s]
            )


def finish(got, full):
    return pl.pallas_call(
        finish_kernel,
        out_shape=jax.ShapeDtypeStruct((LINES, LANES), F32),
        in_specs=[VMEM] * 2,
        out_specs=VMEM,
        compiler_params=params(8),
        name="finish",
    )(got, full)


def summary_kernel(got_ref, coeff_ref, out_ref):
    energy = jnp.sum(got_ref[:, 0, :]) * (1.0 / CELLS)
    out_ref[0] = energy
    out_ref[1] = jnp.max(coeff_ref[21:22, :])
    out_ref[2] = jnp.max(got_ref[:, 1, :])


def summarize(got, coeffs):
    return pl.pallas_call(
        summary_kernel,
        out_shape=jax.ShapeDtypeStruct((3,), F32),
        in_specs=[VMEM] * 2,
        out_specs=pl.BlockSpec(memory_space=pltpu.SMEM),
        compiler_params=params(8),
        name="summary",
    )(got, coeffs)


def swap(x, axis):
    return lax.all_to_all(x, axis, 0, 0, tiled=True)


def shards(fields, residual, past_fields, past_residuals):
    slabs = lax.axis_size("gz")
    pencils = lax.axis_size("gy")
    res = residual.reshape(LINES, LANES)
    fld = fields.reshape(LINES, LANES)
    past_res = past_residuals.reshape(HIST, LINES, LANES)
    past_fld = past_fields.reshape(HIST, LINES, LANES)
    sums = jnp.sum(swap(gram_partial(res, fld, past_res, slabs), "gz"), axis=0)
    sums = swap(jnp.broadcast_to(sums[None], (pencils, 8, LANES)), "gy")
    mixed, ends, coeffs = mix(sums, res, past_res, pencils)
    ends = swap(ends, "gy")
    base, moments = local_part(coeffs, fld, past_fld, mixed)
    full, send = column_part(ends, base, moments, slabs)
    got = swap(send.reshape(slabs, 8, LANES), "gz")
    send = owner_part(got.reshape(slabs * 8, LANES))
    got = swap(send.reshape(slabs, 8, LANES), "gz").reshape(slabs * 8, LANES)
    last = swap(tally(got, pencils), "gy")
    new_fields = finish(got, full)
    return new_fields.reshape(fields.shape), summarize(last, coeffs)


def solution(mesh):
    placed = (
        P(None, "gz", "gy", None),
        P(None, "gz", "gy", None),
        P(None, None, "gz", "gy", None),
        P(None, None, "gz", "gy", None),
    )
    return jax.shard_map(
        shards, mesh=mesh, in_specs=placed, out_specs=(P(None, "gz", "gy", None), P()), check_vma=False
    )
```

```python
import functools
import math

import jax
import jax.numpy as jnp
from jax import lax
from jax.experimental import pallas as pl
from jax.experimental.pallas import tpu as pltpu
from jax.sharding import PartitionSpec as P

CHI_N = 20.0
RIDGE = 0.01
STEP_LOCAL = 0.1
EXACT = lax.Precision.HIGHEST
HIST = 20
BANDS = HIST + 2
LINES = 512
CHUNK = 64
LANES = 128
PLANES = 8
ROWS = 32
F32 = jnp.float32
BF16 = jnp.bfloat16
LENGTH = 256
DECAY = LENGTH / 4.0
TOTAL = sum(math.cosh((0.5 * LENGTH - d) / DECAY) for d in range(LENGTH))
WIDE = math.exp(0.5 * LENGTH / DECAY)
CELLS = 256 * 256 * 128

VMEM = pl.BlockSpec(memory_space=pltpu.VMEM)
HBM = pl.BlockSpec(memory_space=pltpu.HBM)


def params(mib, **more):
    return pltpu.CompilerParams(vmem_limit_bytes=mib * 1024 * 1024, **more)


def halves(x):
    high = x.astype(BF16)
    return high, (x - high.astype(F32)).astype(BF16)


def product(a, b, contract):
    return lax.dot_general(a, b, (contract, ((), ())), preferred_element_type=F32)


def split_product(a, b, contract):
    a_high, a_low = halves(a)
    b_high, b_low = halves(b)
    return (
        product(a_high, b_high, contract)
        + product(a_high, b_low, contract)
        + product(a_low, b_high, contract)
    )


def iota(shape, dim):
    return lax.broadcasted_iota(jnp.int32, shape, dim)


def ramp(shape, dim, sign):
    return jnp.exp(iota(shape, dim).astype(F32) * (sign / DECAY))


def near_matrix(count):
    lag = jnp.abs(iota((count, count), 0) - iota((count, count), 1)).astype(F32)
    half = (0.5 * LENGTH - lag) / DECAY
    return (jnp.exp(half) + jnp.exp(-half)) * (0.5 / TOTAL)


def near_value(lag):
    return math.cosh((0.5 * LENGTH - lag) / DECAY) / TOTAL


def far_weight(row, col, width):
    gap = (row - col).astype(F32) * (width / DECAY)
    below = jnp.exp(-gap) * (WIDE * 0.5 / TOTAL)
    above = jnp.exp(-gap) * (0.5 / (WIDE * TOTAL))
    return jnp.where(col < row, below, jnp.where(col > row, above, 0.0))


def gram_kernel(res_any, fld_any, past_any, out_ref, res_ref, past_ref, fld_ref, high_ref, low_ref, acc_ref, sems):
    steps = LINES // CHUNK
    copies = [
        pltpu.make_async_copy(res_any, res_ref, sems.at[steps]),
        pltpu.make_async_copy(fld_any, fld_ref, sems.at[steps + 1]),
    ]
    chunks = []
    for t in range(steps):
        rows = pl.ds(CHUNK * t, CHUNK)
        chunks.append(pltpu.make_async_copy(past_any.at[:, rows], past_ref.at[:, rows], sems.at[t]))
    for copy in copies + chunks:
        copy.start()
    for copy in copies:
        copy.wait()

    def split(t):
        for k in range(CHUNK // 8):
            rows = slice(CHUNK * t + 8 * k, CHUNK * t + 8 * k + 8)
            res = res_ref[rows, :]
            delta = res[None] - past_ref[:, rows, :]
            band = jnp.concatenate(
                [delta.reshape(HIST * 8, LANES), res, fld_ref[rows, :]], axis=0
            )
            columns = slice(LANES * k, LANES * k + LANES)
            high_ref[t % 2, :, columns], low_ref[t % 2, :, columns] = halves(band)

    def multiply(t):
        high = high_ref[t % 2]
        low = low_ref[t % 2]
        for k, part in enumerate((high, low)):
            value = product(high, part, ((1,), (1,)))
            if t == 0:
                acc_ref[k] = value
            else:
                acc_ref[k] += value

    chunks[0].wait()
    split(0)
    for t in range(steps):
        if t + 1 < steps:
            chunks[t + 1].wait()
            split(t + 1)
        multiply(t)

    size = BANDS * 8
    same = (iota((size, size), 0) & 7) == (iota((size, size), 1) & 7)
    major = jnp.where(same, acc_ref[0] + acc_ref[1], 0.0)
    minor = jnp.where(same, acc_ref[1], 0.0)
    columns = (iota((size, LANES), 0) >> 3 == iota((size, LANES), 1)).astype(F32)
    rows = (iota((24, size), 1) >> 3 == iota((24, size), 0)).astype(F32)
    half = lax.dot(rows, major, precision=EXACT) + lax.dot_general(
        rows, minor, (((1,), (1,)), ((), ())), precision=EXACT
    )
    folded = lax.dot(half, columns, precision=EXACT)
    packed = (
        folded[0:8] + pltpu.roll(folded[8:16], 32, 1) + pltpu.roll(folded[16:24], 64, 1)
    )
    out_ref[...] = jnp.broadcast_to(packed[None], out_ref.shape)


def gram_partial(res, fld, past, copies):
    wide = (CHUNK // 8) * LANES
    return pl.pallas_call(
        gram_kernel,
        out_shape=(
            jax.ShapeDtypeStruct((copies, 8, LANES), F32),
            pltpu.VMEM((LINES, LANES), F32),
            pltpu.VMEM((HIST, LINES, LANES), F32),
        ),
        in_specs=[HBM] * 3,
        out_specs=(VMEM,) * 3,
        scratch_shapes=[
            pltpu.VMEM((LINES, LANES), F32),
            pltpu.VMEM((2, BANDS * 8, wide), BF16),
            pltpu.VMEM((2, BANDS * 8, wide), BF16),
            pltpu.VMEM((2, BANDS * 8, BANDS * 8), F32),
            pltpu.SemaphoreType.DMA((LINES // CHUNK + 2,)),
        ],
        compiler_params=params(54),
        name="gram",
    )(*(pltpu.with_memory_space_constraint(x, pltpu.HBM) for x in (res, fld, past)))


def relay_kernel(got_ref, out_ref):
    total = jnp.sum(got_ref[...], axis=0)
    out_ref[...] = jnp.broadcast_to(total[None], out_ref.shape)


def relay(got, copies):
    return pl.pallas_call(
        relay_kernel,
        out_shape=jax.ShapeDtypeStruct((copies, 8, LANES), F32),
        in_specs=[VMEM],
        out_specs=VMEM,
        compiler_params=params(4),
        name="relay",
    )(got)


def solve(packed):
    place = iota((24, LANES), 0)

    def column(i):
        parts = [
            jnp.broadcast_to(packed[:, 32 * b + i : 32 * b + i + 1], (8, LANES)) for b in range(3)
        ]
        return jnp.concatenate(parts, axis=0)

    rows = [column(i) for i in range(HIST)]
    right = column(HIST)
    trace = rows[0][0:1]
    for i in range(1, HIST):
        trace = trace + rows[i][i : i + 1]
    shift = (RIDGE / HIST) * trace + 1.0
    rows = [rows[i] + jnp.where(place == i, shift, 0.0) for i in range(HIST)]
    inverse = []
    for k in range(HIST):
        inv = 1.0 / rows[k][k : k + 1]
        inverse.append(inv)
        after = jnp.where(place > k, rows[k] * inv, 0.0)
        for i in range(k + 1, HIST):
            rows[i] = rows[i] - after * rows[i][k : k + 1]
        right = right - after * right[k : k + 1]
    coeffs = [None] * HIST
    for k in reversed(range(HIST)):
        coeffs[k] = right[k : k + 1] * inverse[k]
        right = right - jnp.where(place < k, rows[k] * coeffs[k], 0.0)
    remain = 1.0 - functools.reduce(jnp.add, coeffs)
    return remain, coeffs


def mix_kernel(
    sums_ref, res_ref, past_ref, fld_ref, past_fld_ref,
    end_ref, ratio_ref, base_ref, moment_ref, mixed_ref, near_ref,
):
    packed = jnp.sum(sums_ref[...], axis=0)
    remain, coeffs = solve(packed)
    res_square = packed[4:5, 64 + HIST : 65 + HIST]
    fld_square = packed[5:6, 65 + HIST : 66 + HIST]
    ratio = jnp.sqrt(res_square / (fld_square + 1.0))
    ratio_ref[...] = jnp.broadcast_to(ratio, ratio_ref.shape)
    coeffs = [jnp.broadcast_to(c, (ROWS, LANES)) for c in coeffs]
    remain = jnp.broadcast_to(remain, (ROWS, LANES))
    rise = ramp((ROWS, LANES), 0, 1.0)
    fall = ramp((ROWS, LANES), 0, -1.0)
    peak = jnp.zeros((ROWS, LANES), F32)
    for plane in range(2 * PLANES):
        rows = slice(ROWS * plane, ROWS * plane + ROWS)
        total = remain * res_ref[rows, :]
        for i in range(HIST):
            total = total + coeffs[i] * past_ref[i, rows, :]
        mixed_ref[:, LANES * plane : LANES * plane + LANES] = total
        peak = jnp.maximum(peak, jnp.abs(total))
        s, z = divmod(plane, PLANES)
        end_ref[0, s, z : z + 1, :] = jnp.sum(rise * total, axis=0, keepdims=True)
        end_ref[0, 2 + s, z : z + 1, :] = jnp.sum(fall * total, axis=0, keepdims=True)
    for k in range(1, end_ref.shape[0]):
        end_ref[k] = end_ref[0]
    moment_ref[4] = peak

    near_ref[...] = split_product(near_matrix(ROWS), mixed_ref[...], ((1,), (0,)))
    for s in range(2):
        near = lambda z: near_ref[:, LANES * (PLANES * s + z) : LANES * (PLANES * s + z + 1)]
        planes = [near(z) for z in range(PLANES)]
        rising = planes[0]
        falling = planes[0]
        for z in range(1, PLANES):
            rising = rising + math.exp(z / DECAY) * planes[z]
            falling = falling + math.exp(-z / DECAY) * planes[z]
        moment_ref[s] = rising
        moment_ref[2 + s] = falling
        for z in range(PLANES):
            plane = PLANES * s + z
            rows = slice(ROWS * plane, ROWS * plane + ROWS)
            total = STEP_LOCAL * mixed_ref[:, LANES * plane : LANES * plane + LANES]
            total = total + remain * fld_ref[rows, :]
            for i in range(HIST):
                total = total + coeffs[i] * past_fld_ref[i, rows, :]
            for z2 in range(PLANES):
                total = total + near_value(abs(z - z2)) * planes[z2]
            base_ref[rows, :] = total


def mix(sums, res, past, fld, past_fld, copies):
    return pl.pallas_call(
        mix_kernel,
        out_shape=(
            jax.ShapeDtypeStruct((copies, 4, PLANES, LANES), F32),
            jax.ShapeDtypeStruct((8, LANES), F32),
            jax.ShapeDtypeStruct((LINES, LANES), F32),
            jax.ShapeDtypeStruct((5, ROWS, LANES), F32),
        ),
        in_specs=[VMEM] * 5,
        out_specs=(VMEM,) * 4,
        scratch_shapes=[
            pltpu.VMEM((ROWS, 2 * PLANES * LANES), F32),
            pltpu.VMEM((ROWS, 2 * PLANES * LANES), F32),
        ],
        compiler_params=params(14),
        name="mix",
    )(sums, res, past, fld, past_fld)


def column_kernel(ends_ref, base_ref, moment_ref, full_ref, send_ref):
    here = lax.axis_index("gy")
    count = ends_ref.shape[0]
    shape = (count, LANES)
    other = iota(shape, 0)
    down = far_weight(jnp.full(shape, here, jnp.int32), other, ROWS)
    up = far_weight(other, jnp.full(shape, here, jnp.int32), ROWS)
    fields = []
    for kind, weight in ((0, down), (2, up)):
        for s in range(2):
            total = weight[0:1] * ends_ref[0, kind + s]
            for q in range(1, count):
                total = total + weight[q : q + 1] * ends_ref[q, kind + s]
            fields.append(total)
    wide = jnp.concatenate(fields, axis=1)
    row = iota((16, PLANES), 0)
    col = iota((16, PLANES), 1)
    lag = (0.5 * LENGTH - jnp.abs(row - col).astype(F32)) / DECAY
    near = (jnp.exp(lag) + jnp.exp(-lag)) * (0.5 / TOTAL)
    rise = jnp.exp(col.astype(F32) / DECAY)
    fall = jnp.exp(col.astype(F32) / -DECAY)
    mixer = jnp.where(row < 8, near, jnp.where(row == 8, rise, fall))
    smooth = lax.dot(mixer, wide, precision=EXACT)

    fall_y = ramp((ROWS, LANES), 0, -1.0)
    rise_y = ramp((ROWS, LANES), 0, 1.0)

    def spread(line, s):
        return (
            fall_y * smooth[line : line + 1, LANES * s : LANES * s + LANES]
            + rise_y * smooth[line : line + 1, LANES * (2 + s) : LANES * (2 + s) + LANES]
        )

    def put(k, value):
        send_ref[pl.ds(k, ROWS, stride=8), :] = value

    for s in range(2):
        put(s, moment_ref[s] + spread(8, s))
        put(2 + s, moment_ref[2 + s] + spread(9, s))
    first = jnp.zeros((ROWS, LANES), F32)
    second = jnp.zeros((ROWS, LANES), F32)
    energy = jnp.zeros((ROWS, LANES), F32)
    for z in range(PLANES):
        pair = []
        for s in range(2):
            rows = slice(ROWS * (PLANES * s + z), ROWS * (PLANES * s + z) + ROWS)
            value = base_ref[rows, :] + spread(z, s)
            full_ref[rows, :] = value
            pair.append(value)
        gap = pair[0] - pair[1]
        first = first + math.exp(-z / DECAY) * gap
        second = second + math.exp(z / DECAY) * gap
        energy = energy + (gap * gap * (1.0 / (4.0 * CHI_N)) - 0.5 * (pair[0] + pair[1]))
    put(4, first)
    put(5, second)
    put(6, energy)
    put(7, moment_ref[4])


def column_part(ends, base, moments, owners):
    return pl.pallas_call(
        column_kernel,
        out_shape=(
            jax.ShapeDtypeStruct((LINES, LANES), F32),
            jax.ShapeDtypeStruct((owners * 8, LANES), F32),
        ),
        in_specs=[VMEM] * 3,
        out_specs=(VMEM,) * 2,
        compiler_params=params(8),
        name="column_part",
    )(ends, base, moments)


def owner_kernel(got_ref, send_ref):
    count = got_ref.shape[0] // 8
    take = lambda k: got_ref[pl.ds(k, count, stride=8), :]
    row = iota((count, count), 0)
    col = iota((count, count), 1)
    rising = jnp.concatenate([take(0), take(1)], axis=1)
    falling = jnp.concatenate([take(2), take(3)], axis=1)
    down = split_product(far_weight(row, col, PLANES), rising, ((1,), (0,)))
    up = split_product(far_weight(col, row, PLANES), falling, ((1,), (0,)))
    down = (down[:, :LANES], down[:, LANES:])
    up = (up[:, :LANES], up[:, LANES:])
    fall_sum = sum(math.exp(-z / DECAY) for z in range(PLANES))
    rise_sum = sum(math.exp(z / DECAY) for z in range(PLANES))
    fall_square = sum(math.exp(-2.0 * z / DECAY) for z in range(PLANES))
    rise_square = sum(math.exp(2.0 * z / DECAY) for z in range(PLANES))
    a = down[0] - down[1]
    b = up[0] - up[1]
    square = (
        a * (2.0 * take(4) + fall_square * a + (2.0 * PLANES) * b)
        + b * (2.0 * take(5) + rise_square * b)
    )
    energy = (
        take(6)
        + square * (1.0 / (4.0 * CHI_N))
        - 0.5 * (fall_sum * (down[0] + down[1]) + rise_sum * (up[0] + up[1]))
    )
    energy = jnp.sum(energy, axis=0, keepdims=True)
    peak = jnp.max(take(7), axis=0, keepdims=True)
    values = (*down, *up, energy, peak, peak, peak)
    for k, value in enumerate(values):
        send_ref[pl.ds(k, count, stride=8), :] = jnp.broadcast_to(value, (count, LANES))


def owner_part(got):
    return pl.pallas_call(
        owner_kernel,
        out_shape=jax.ShapeDtypeStruct(got.shape, F32),
        in_specs=[VMEM],
        out_specs=VMEM,
        compiler_params=params(8),
        name="owner_part",
    )(got)


def tally_kernel(got_ref, out_ref):
    energy = jnp.sum(got_ref[pl.ds(4, ROWS, stride=8), :], axis=0, keepdims=True)
    peak = jnp.max(got_ref[pl.ds(5, ROWS, stride=8), :], axis=0, keepdims=True)
    value = jnp.where(iota((8, LANES), 0) == 0, energy, peak)
    out_ref[...] = jnp.broadcast_to(value[None], out_ref.shape)


def tally(got, copies):
    return pl.pallas_call(
        tally_kernel,
        out_shape=jax.ShapeDtypeStruct((copies, 8, LANES), F32),
        in_specs=[VMEM],
        out_specs=VMEM,
        compiler_params=params(8),
        name="tally",
    )(got)


def finish_kernel(last_ref, got_ref, full_ref, ratio_ref, out_ref, summary_ref):
    down = [got_ref[pl.ds(s, ROWS, stride=8), :] for s in range(2)]
    up = [got_ref[pl.ds(2 + s, ROWS, stride=8), :] for s in range(2)]
    for s in range(2):
        for z in range(PLANES):
            rows = slice(ROWS * (PLANES * s + z), ROWS * (PLANES * s + z) + ROWS)
            out_ref[rows, :] = (
                full_ref[rows, :]
                + math.exp(-z / DECAY) * down[s]
                + math.exp(z / DECAY) * up[s]
            )
    summary_ref[0] = jnp.sum(last_ref[:, 0, :]) * (1.0 / CELLS)
    summary_ref[1] = jnp.max(ratio_ref[...])
    summary_ref[2] = jnp.max(last_ref[:, 1, :])


def finish(last, got, full, ratio):
    return pl.pallas_call(
        finish_kernel,
        out_shape=(
            jax.ShapeDtypeStruct((LINES, LANES), F32),
            jax.ShapeDtypeStruct((3,), F32),
        ),
        in_specs=[VMEM] * 4,
        out_specs=(VMEM, pl.BlockSpec(memory_space=pltpu.SMEM)),
        compiler_params=params(8),
        name="finish",
    )(last, got, full, ratio)


def swap(x, axis):
    return lax.all_to_all(x, axis, 0, 0, tiled=True)


def shards(fields, residual, past_fields, past_residuals):
    slabs = lax.axis_size("gz")
    pencils = lax.axis_size("gy")
    res = residual.reshape(LINES, LANES)
    fld = fields.reshape(LINES, LANES)
    past_res = past_residuals.reshape(HIST, LINES, LANES)
    past_fld = past_fields.reshape(HIST, LINES, LANES)
    sums, res, past_res = gram_partial(res, fld, past_res, slabs)
    sums = swap(relay(swap(sums, "gz"), pencils), "gy")
    ends, ratio, base, moments = mix(sums, res, past_res, fld, past_fld, pencils)
    ends = swap(ends, "gy")
    full, send = column_part(ends, base, moments, slabs)
    got = swap(send.reshape(slabs, 8, LANES), "gz")
    send = owner_part(got.reshape(slabs * 8, LANES))
    got = swap(send.reshape(slabs, 8, LANES), "gz").reshape(slabs * 8, LANES)
    last = swap(tally(got, pencils), "gy")
    new_fields, summary = finish(last, got, full, ratio)
    return new_fields.reshape(fields.shape), summary


def solution(mesh):
    placed = (
        P(None, "gz", "gy", None),
        P(None, "gz", "gy", None),
        P(None, None, "gz", "gy", None),
        P(None, None, "gz", "gy", None),
    )
    return jax.shard_map(
        shards, mesh=mesh, in_specs=placed, out_specs=(P(None, "gz", "gy", None), P()), check_vma=False
    )
```

```python
import functools
import math

import jax
import jax.numpy as jnp
from jax import lax
from jax.experimental import pallas as pl
from jax.experimental.pallas import tpu as pltpu
from jax.sharding import PartitionSpec as P

CHI_N = 20.0
RIDGE = 0.01
STEP_LOCAL = 0.1
EXACT = lax.Precision.HIGHEST
HIST = 20
BANDS = HIST + 2
LINES = 512
CHUNK = 64
LANES = 128
PLANES = 8
ROWS = 32
F32 = jnp.float32
BF16 = jnp.bfloat16
LENGTH = 256
DECAY = LENGTH / 4.0
TOTAL = sum(math.cosh((0.5 * LENGTH - d) / DECAY) for d in range(LENGTH))
WIDE = math.exp(0.5 * LENGTH / DECAY)
CELLS = 256 * 256 * 128

VMEM = pl.BlockSpec(memory_space=pltpu.VMEM)
HBM = pl.BlockSpec(memory_space=pltpu.HBM)


def params(mib, **more):
    return pltpu.CompilerParams(vmem_limit_bytes=mib * 1024 * 1024, **more)


def halves(x):
    high = x.astype(BF16)
    return high, (x - high.astype(F32)).astype(BF16)


def product(a, b, contract):
    return lax.dot_general(a, b, (contract, ((), ())), preferred_element_type=F32)


def split_product(a, b, contract):
    a_high, a_low = halves(a)
    b_high, b_low = halves(b)
    return (
        product(a_high, b_high, contract)
        + product(a_high, b_low, contract)
        + product(a_low, b_high, contract)
    )


def iota(shape, dim):
    return lax.broadcasted_iota(jnp.int32, shape, dim)


def ramp(shape, dim, sign):
    return jnp.exp(iota(shape, dim).astype(F32) * (sign / DECAY))


def near_matrix(count):
    lag = jnp.abs(iota((count, count), 0) - iota((count, count), 1)).astype(F32)
    half = (0.5 * LENGTH - lag) / DECAY
    return (jnp.exp(half) + jnp.exp(-half)) * (0.5 / TOTAL)


def near_value(lag):
    return math.cosh((0.5 * LENGTH - lag) / DECAY) / TOTAL


def far_weight(row, col, width):
    gap = (row - col).astype(F32) * (width / DECAY)
    below = jnp.exp(-gap) * (WIDE * 0.5 / TOTAL)
    above = jnp.exp(-gap) * (0.5 / (WIDE * TOTAL))
    return jnp.where(col < row, below, jnp.where(col > row, above, 0.0))


def gram_kernel(res_any, fld_any, past_any, out_ref, res_ref, past_ref, fld_ref, high_ref, low_ref, acc_ref, sems):
    steps = LINES // CHUNK
    copies = [
        pltpu.make_async_copy(res_any, res_ref, sems.at[steps]),
        pltpu.make_async_copy(fld_any, fld_ref, sems.at[steps + 1]),
    ]
    chunks = []
    for t in range(steps):
        rows = pl.ds(CHUNK * t, CHUNK)
        chunks.append(pltpu.make_async_copy(past_any.at[:, rows], past_ref.at[:, rows], sems.at[t]))
    for copy in copies + chunks:
        copy.start()
    for copy in copies:
        copy.wait()

    def split(t):
        for k in range(CHUNK // 8):
            rows = slice(CHUNK * t + 8 * k, CHUNK * t + 8 * k + 8)
            res = res_ref[rows, :]
            delta = res[None] - past_ref[:, rows, :]
            band = jnp.concatenate(
                [delta.reshape(HIST * 8, LANES), res, fld_ref[rows, :]], axis=0
            )
            columns = slice(LANES * k, LANES * k + LANES)
            high_ref[t % 2, :, columns], low_ref[t % 2, :, columns] = halves(band)

    def multiply(t):
        high = high_ref[t % 2]
        low = low_ref[t % 2]
        for k, part in enumerate((high, low)):
            value = product(high, part, ((1,), (1,)))
            if t == 0:
                acc_ref[k] = value
            else:
                acc_ref[k] += value

    chunks[0].wait()
    split(0)
    for t in range(steps):
        if t + 1 < steps:
            chunks[t + 1].wait()
            split(t + 1)
        multiply(t)

    size = BANDS * 8
    same = (iota((size, size), 0) & 7) == (iota((size, size), 1) & 7)
    major = jnp.where(same, acc_ref[0] + acc_ref[1], 0.0)
    minor = jnp.where(same, acc_ref[1], 0.0)
    columns = (iota((size, LANES), 0) >> 3 == iota((size, LANES), 1)).astype(F32)
    rows = (iota((24, size), 1) >> 3 == iota((24, size), 0)).astype(F32)
    half = lax.dot(rows, major, precision=EXACT) + lax.dot_general(
        rows, minor, (((1,), (1,)), ((), ())), precision=EXACT
    )
    folded = lax.dot(half, columns, precision=EXACT)
    packed = (
        folded[0:8] + pltpu.roll(folded[8:16], 32, 1) + pltpu.roll(folded[16:24], 64, 1)
    )
    out_ref[...] = jnp.broadcast_to(packed[None], out_ref.shape)


def gram_partial(res, fld, past, copies):
    wide = (CHUNK // 8) * LANES
    return pl.pallas_call(
        gram_kernel,
        out_shape=(
            jax.ShapeDtypeStruct((copies, 8, LANES), F32),
            pltpu.VMEM((LINES, LANES), F32),
            pltpu.VMEM((HIST, LINES, LANES), F32),
        ),
        in_specs=[HBM] * 3,
        out_specs=(VMEM,) * 3,
        scratch_shapes=[
            pltpu.VMEM((LINES, LANES), F32),
            pltpu.VMEM((2, BANDS * 8, wide), BF16),
            pltpu.VMEM((2, BANDS * 8, wide), BF16),
            pltpu.VMEM((2, BANDS * 8, BANDS * 8), F32),
            pltpu.SemaphoreType.DMA((LINES // CHUNK + 2,)),
        ],
        compiler_params=params(4),
        name="gram",
    )(*(pltpu.with_memory_space_constraint(x, pltpu.HBM) for x in (res, fld, past)))


def relay_kernel(got_ref, out_ref):
    total = jnp.sum(got_ref[...], axis=0)
    out_ref[...] = jnp.broadcast_to(total[None], out_ref.shape)


def relay(got, copies):
    return pl.pallas_call(
        relay_kernel,
        out_shape=jax.ShapeDtypeStruct((copies, 8, LANES), F32),
        in_specs=[VMEM],
        out_specs=VMEM,
        compiler_params=params(4),
        cost_estimate=pl.CostEstimate(flops=5_000_000_000, bytes_accessed=163840, transcendentals=0),
        name="relay",
    )(got)


def solve(packed):
    place = iota((24, LANES), 0)

    def column(i):
        parts = [
            jnp.broadcast_to(packed[:, 32 * b + i : 32 * b + i + 1], (8, LANES)) for b in range(3)
        ]
        return jnp.concatenate(parts, axis=0)

    rows = [column(i) for i in range(HIST)]
    right = column(HIST)
    trace = rows[0][0:1]
    for i in range(1, HIST):
        trace = trace + rows[i][i : i + 1]
    shift = (RIDGE / HIST) * trace + 1.0
    rows = [rows[i] + jnp.where(place == i, shift, 0.0) for i in range(HIST)]
    inverse = []
    for k in range(HIST):
        inv = 1.0 / rows[k][k : k + 1]
        inverse.append(inv)
        after = jnp.where(place > k, rows[k] * inv, 0.0)
        for i in range(k + 1, HIST):
            rows[i] = rows[i] - after * rows[i][k : k + 1]
        right = right - after * right[k : k + 1]
    coeffs = [None] * HIST
    for k in reversed(range(HIST)):
        coeffs[k] = right[k : k + 1] * inverse[k]
        right = right - jnp.where(place < k, rows[k] * coeffs[k], 0.0)
    remain = 1.0 - functools.reduce(jnp.add, coeffs)
    return remain, coeffs


def mix_kernel(
    sums_ref, res_ref, past_ref, fld_ref, past_fld_ref,
    end_ref, ratio_ref, base_ref, moment_ref, mixed_ref, near_ref,
):
    packed = jnp.sum(sums_ref[...], axis=0)
    remain, coeffs = solve(packed)
    res_square = packed[4:5, 64 + HIST : 65 + HIST]
    fld_square = packed[5:6, 65 + HIST : 66 + HIST]
    ratio = jnp.sqrt(res_square / (fld_square + 1.0))
    ratio_ref[...] = jnp.broadcast_to(ratio, ratio_ref.shape)
    coeffs = [jnp.broadcast_to(c, (ROWS, LANES)) for c in coeffs]
    remain = jnp.broadcast_to(remain, (ROWS, LANES))
    rise = ramp((ROWS, LANES), 0, 1.0)
    fall = ramp((ROWS, LANES), 0, -1.0)
    peak = jnp.zeros((ROWS, LANES), F32)
    for plane in range(2 * PLANES):
        rows = slice(ROWS * plane, ROWS * plane + ROWS)
        total = remain * res_ref[rows, :]
        for i in range(HIST):
            total = total + coeffs[i] * past_ref[i, rows, :]
        mixed_ref[:, LANES * plane : LANES * plane + LANES] = total
        peak = jnp.maximum(peak, jnp.abs(total))
        s, z = divmod(plane, PLANES)
        end_ref[0, s, z : z + 1, :] = jnp.sum(rise * total, axis=0, keepdims=True)
        end_ref[0, 2 + s, z : z + 1, :] = jnp.sum(fall * total, axis=0, keepdims=True)
    for k in range(1, end_ref.shape[0]):
        end_ref[k] = end_ref[0]
    moment_ref[4] = peak

    near_ref[...] = split_product(near_matrix(ROWS), mixed_ref[...], ((1,), (0,)))
    for s in range(2):
        near = lambda z: near_ref[:, LANES * (PLANES * s + z) : LANES * (PLANES * s + z + 1)]
        planes = [near(z) for z in range(PLANES)]
        rising = planes[0]
        falling = planes[0]
        for z in range(1, PLANES):
            rising = rising + math.exp(z / DECAY) * planes[z]
            falling = falling + math.exp(-z / DECAY) * planes[z]
        moment_ref[s] = rising
        moment_ref[2 + s] = falling
        for z in range(PLANES):
            plane = PLANES * s + z
            rows = slice(ROWS * plane, ROWS * plane + ROWS)
            total = STEP_LOCAL * mixed_ref[:, LANES * plane : LANES * plane + LANES]
            total = total + remain * fld_ref[rows, :]
            for i in range(HIST):
                total = total + coeffs[i] * past_fld_ref[i, rows, :]
            for z2 in range(PLANES):
                total = total + near_value(abs(z - z2)) * planes[z2]
            base_ref[rows, :] = total


def mix(sums, res, past, fld, past_fld, copies):
    return pl.pallas_call(
        mix_kernel,
        out_shape=(
            jax.ShapeDtypeStruct((copies, 4, PLANES, LANES), F32),
            jax.ShapeDtypeStruct((8, LANES), F32),
            jax.ShapeDtypeStruct((LINES, LANES), F32),
            jax.ShapeDtypeStruct((5, ROWS, LANES), F32),
        ),
        in_specs=[VMEM] * 5,
        out_specs=(VMEM,) * 4,
        scratch_shapes=[
            pltpu.VMEM((ROWS, 2 * PLANES * LANES), F32),
            pltpu.VMEM((ROWS, 2 * PLANES * LANES), F32),
        ],
        compiler_params=params(14),
        name="mix",
    )(sums, res, past, fld, past_fld)


def column_kernel(ends_ref, base_ref, moment_ref, full_ref, send_ref):
    here = lax.axis_index("gy")
    count = ends_ref.shape[0]
    shape = (count, LANES)
    other = iota(shape, 0)
    down = far_weight(jnp.full(shape, here, jnp.int32), other, ROWS)
    up = far_weight(other, jnp.full(shape, here, jnp.int32), ROWS)
    fields = []
    for kind, weight in ((0, down), (2, up)):
        for s in range(2):
            total = weight[0:1] * ends_ref[0, kind + s]
            for q in range(1, count):
                total = total + weight[q : q + 1] * ends_ref[q, kind + s]
            fields.append(total)
    wide = jnp.concatenate(fields, axis=1)
    row = iota((16, PLANES), 0)
    col = iota((16, PLANES), 1)
    lag = (0.5 * LENGTH - jnp.abs(row - col).astype(F32)) / DECAY
    near = (jnp.exp(lag) + jnp.exp(-lag)) * (0.5 / TOTAL)
    rise = jnp.exp(col.astype(F32) / DECAY)
    fall = jnp.exp(col.astype(F32) / -DECAY)
    mixer = jnp.where(row < 8, near, jnp.where(row == 8, rise, fall))
    smooth = lax.dot(mixer, wide, precision=EXACT)

    fall_y = ramp((ROWS, LANES), 0, -1.0)
    rise_y = ramp((ROWS, LANES), 0, 1.0)

    def spread(line, s):
        return (
            fall_y * smooth[line : line + 1, LANES * s : LANES * s + LANES]
            + rise_y * smooth[line : line + 1, LANES * (2 + s) : LANES * (2 + s) + LANES]
        )

    def put(k, value):
        send_ref[pl.ds(k, ROWS, stride=8), :] = value

    for s in range(2):
        put(s, moment_ref[s] + spread(8, s))
        put(2 + s, moment_ref[2 + s] + spread(9, s))
    first = jnp.zeros((ROWS, LANES), F32)
    second = jnp.zeros((ROWS, LANES), F32)
    energy = jnp.zeros((ROWS, LANES), F32)
    for z in range(PLANES):
        pair = []
        for s in range(2):
            rows = slice(ROWS * (PLANES * s + z), ROWS * (PLANES * s + z) + ROWS)
            value = base_ref[rows, :] + spread(z, s)
            full_ref[rows, :] = value
            pair.append(value)
        gap = pair[0] - pair[1]
        first = first + math.exp(-z / DECAY) * gap
        second = second + math.exp(z / DECAY) * gap
        energy = energy + (gap * gap * (1.0 / (4.0 * CHI_N)) - 0.5 * (pair[0] + pair[1]))
    put(4, first)
    put(5, second)
    put(6, energy)
    put(7, moment_ref[4])


def column_part(ends, base, moments, owners):
    return pl.pallas_call(
        column_kernel,
        out_shape=(
            jax.ShapeDtypeStruct((LINES, LANES), F32),
            jax.ShapeDtypeStruct((owners * 8, LANES), F32),
        ),
        in_specs=[VMEM] * 3,
        out_specs=(VMEM,) * 2,
        compiler_params=params(8),
        name="column_part",
    )(ends, base, moments)


def owner_kernel(got_ref, send_ref):
    count = got_ref.shape[0] // 8
    take = lambda k: got_ref[pl.ds(k, count, stride=8), :]
    row = iota((count, count), 0)
    col = iota((count, count), 1)
    rising = jnp.concatenate([take(0), take(1)], axis=1)
    falling = jnp.concatenate([take(2), take(3)], axis=1)
    down = split_product(far_weight(row, col, PLANES), rising, ((1,), (0,)))
    up = split_product(far_weight(col, row, PLANES), falling, ((1,), (0,)))
    down = (down[:, :LANES], down[:, LANES:])
    up = (up[:, :LANES], up[:, LANES:])
    fall_sum = sum(math.exp(-z / DECAY) for z in range(PLANES))
    rise_sum = sum(math.exp(z / DECAY) for z in range(PLANES))
    fall_square = sum(math.exp(-2.0 * z / DECAY) for z in range(PLANES))
    rise_square = sum(math.exp(2.0 * z / DECAY) for z in range(PLANES))
    a = down[0] - down[1]
    b = up[0] - up[1]
    square = (
        a * (2.0 * take(4) + fall_square * a + (2.0 * PLANES) * b)
        + b * (2.0 * take(5) + rise_square * b)
    )
    energy = (
        take(6)
        + square * (1.0 / (4.0 * CHI_N))
        - 0.5 * (fall_sum * (down[0] + down[1]) + rise_sum * (up[0] + up[1]))
    )
    energy = jnp.sum(energy, axis=0, keepdims=True)
    peak = jnp.max(take(7), axis=0, keepdims=True)
    values = (*down, *up, energy, peak, peak, peak)
    for k, value in enumerate(values):
        send_ref[pl.ds(k, count, stride=8), :] = jnp.broadcast_to(value, (count, LANES))


def owner_part(got):
    return pl.pallas_call(
        owner_kernel,
        out_shape=jax.ShapeDtypeStruct(got.shape, F32),
        in_specs=[VMEM],
        out_specs=VMEM,
        compiler_params=params(8),
        name="owner_part",
    )(got)


def tally_kernel(got_ref, out_ref):
    energy = jnp.sum(got_ref[pl.ds(4, ROWS, stride=8), :], axis=0, keepdims=True)
    peak = jnp.max(got_ref[pl.ds(5, ROWS, stride=8), :], axis=0, keepdims=True)
    value = jnp.where(iota((8, LANES), 0) == 0, energy, peak)
    out_ref[...] = jnp.broadcast_to(value[None], out_ref.shape)


def tally(got, copies):
    return pl.pallas_call(
        tally_kernel,
        out_shape=jax.ShapeDtypeStruct((copies, 8, LANES), F32),
        in_specs=[VMEM],
        out_specs=VMEM,
        compiler_params=params(8),
        name="tally",
    )(got)


def finish_kernel(last_ref, got_ref, full_ref, ratio_ref, out_ref, summary_ref):
    down = [got_ref[pl.ds(s, ROWS, stride=8), :] for s in range(2)]
    up = [got_ref[pl.ds(2 + s, ROWS, stride=8), :] for s in range(2)]
    for s in range(2):
        for z in range(PLANES):
            rows = slice(ROWS * (PLANES * s + z), ROWS * (PLANES * s + z) + ROWS)
            out_ref[rows, :] = (
                full_ref[rows, :]
                + math.exp(-z / DECAY) * down[s]
                + math.exp(z / DECAY) * up[s]
            )
    summary_ref[0] = jnp.sum(last_ref[:, 0, :]) * (1.0 / CELLS)
    summary_ref[1] = jnp.max(ratio_ref[...])
    summary_ref[2] = jnp.max(last_ref[:, 1, :])


def finish(last, got, full, ratio):
    return pl.pallas_call(
        finish_kernel,
        out_shape=(
            jax.ShapeDtypeStruct((LINES, LANES), F32),
            jax.ShapeDtypeStruct((3,), F32),
        ),
        in_specs=[VMEM] * 4,
        out_specs=(VMEM, pl.BlockSpec(memory_space=pltpu.SMEM)),
        compiler_params=params(8),
        name="finish",
    )(last, got, full, ratio)


def swap(x, axis):
    return lax.all_to_all(x, axis, 0, 0, tiled=True)


def shards(fields, residual, past_fields, past_residuals):
    slabs = lax.axis_size("gz")
    pencils = lax.axis_size("gy")
    res = residual.reshape(LINES, LANES)
    fld = fields.reshape(LINES, LANES)
    past_res = past_residuals.reshape(HIST, LINES, LANES)
    past_fld = past_fields.reshape(HIST, LINES, LANES)
    sums, res, past_res = gram_partial(res, fld, past_res, slabs)
    sums = swap(relay(swap(sums, "gz"), pencils), "gy")
    ends, ratio, base, moments = mix(sums, res, past_res, fld, past_fld, pencils)
    ends = swap(ends, "gy")
    full, send = column_part(ends, base, moments, slabs)
    got = swap(send.reshape(slabs, 8, LANES), "gz")
    send = owner_part(got.reshape(slabs * 8, LANES))
    got = swap(send.reshape(slabs, 8, LANES), "gz").reshape(slabs * 8, LANES)
    last = swap(tally(got, pencils), "gy")
    new_fields, summary = finish(last, got, full, ratio)
    return new_fields.reshape(fields.shape), summary


def solution(mesh):
    placed = (
        P(None, "gz", "gy", None),
        P(None, "gz", "gy", None),
        P(None, None, "gz", "gy", None),
        P(None, None, "gz", "gy", None),
    )
    return jax.shard_map(
        shards, mesh=mesh, in_specs=placed, out_specs=(P(None, "gz", "gy", None), P()), check_vma=False
    )
```

```python
import functools
import math

import jax
import jax.numpy as jnp
from jax import lax
from jax.experimental import pallas as pl
from jax.experimental.pallas import tpu as pltpu
from jax.sharding import PartitionSpec as P

CHI_N = 20.0
RIDGE = 0.01
STEP_LOCAL = 0.1
EXACT = lax.Precision.HIGHEST
HIST = 20
BANDS = HIST + 2
LINES = 512
CHUNK = 64
AHEAD = 3
LANES = 128
PLANES = 8
ROWS = 32
F32 = jnp.float32
BF16 = jnp.bfloat16
LENGTH = 256
DECAY = LENGTH / 4.0
TOTAL = sum(math.cosh((0.5 * LENGTH - d) / DECAY) for d in range(LENGTH))
WIDE = math.exp(0.5 * LENGTH / DECAY)
CELLS = 256 * 256 * 128

VMEM = pl.BlockSpec(memory_space=pltpu.VMEM)
HBM = pl.BlockSpec(memory_space=pltpu.HBM)


def params(mib, **more):
    return pltpu.CompilerParams(vmem_limit_bytes=mib * 1024 * 1024, **more)


def halves(x):
    high = x.astype(BF16)
    return high, (x - high.astype(F32)).astype(BF16)


def product(a, b, contract):
    return lax.dot_general(a, b, (contract, ((), ())), preferred_element_type=F32)


def split_product(a, b, contract):
    a_high, a_low = halves(a)
    b_high, b_low = halves(b)
    return (
        product(a_high, b_high, contract)
        + product(a_high, b_low, contract)
        + product(a_low, b_high, contract)
    )


def iota(shape, dim):
    return lax.broadcasted_iota(jnp.int32, shape, dim)


def ramp(shape, dim, sign):
    return jnp.exp(iota(shape, dim).astype(F32) * (sign / DECAY))


def near_matrix(count):
    lag = jnp.abs(iota((count, count), 0) - iota((count, count), 1)).astype(F32)
    half = (0.5 * LENGTH - lag) / DECAY
    return (jnp.exp(half) + jnp.exp(-half)) * (0.5 / TOTAL)


def near_value(lag):
    return math.cosh((0.5 * LENGTH - lag) / DECAY) / TOTAL


def far_weight(row, col, width):
    gap = (row - col).astype(F32) * (width / DECAY)
    below = jnp.exp(-gap) * (WIDE * 0.5 / TOTAL)
    above = jnp.exp(-gap) * (0.5 / (WIDE * TOTAL))
    return jnp.where(col < row, below, jnp.where(col > row, above, 0.0))


def thirds(x):
    high, rest = halves(x)
    rest = x - high.astype(F32)
    middle, low = halves(rest)
    return high, middle, low


def select(picker, x, contract):
    return functools.reduce(jnp.add, (product(picker, part, contract) for part in thirds(x)))


def gram_kernel(ahead, res_any, fld_any, past_any, out_ref, res_ref, past_ref, fld_ref, high_ref, low_ref, acc_ref, sems):
    steps = LINES // CHUNK
    copies = [
        pltpu.make_async_copy(res_any, res_ref, sems.at[steps]),
        pltpu.make_async_copy(fld_any, fld_ref, sems.at[steps + 1]),
    ]

    def chunk(t):
        rows = pl.ds(CHUNK * t, CHUNK)
        return pltpu.make_async_copy(past_any.at[:, rows], past_ref.at[:, rows], sems.at[t])

    for copy in copies:
        copy.start()
    for t in range(ahead):
        chunk(t).start()
    acc_ref[...] = jnp.zeros_like(acc_ref)
    for copy in copies:
        copy.wait()

    def split(t):
        slot = t & 1
        for k in range(CHUNK // 8):
            rows = pl.ds(pl.multiple_of(CHUNK * t + 8 * k, 8), 8)
            res = res_ref[rows, :]
            delta = res[None] - past_ref[:, rows, :]
            band = jnp.concatenate(
                [delta.reshape(HIST * 8, LANES), res, fld_ref[rows, :]], axis=0
            )
            columns = slice(LANES * k, LANES * k + LANES)
            high_ref[slot, :, columns], low_ref[slot, :, columns] = halves(band)

    def multiply(t):
        slot = t & 1
        high = high_ref[slot]
        acc_ref[0] += product(high, high, ((1,), (1,)))
        acc_ref[1] += product(high, low_ref[slot], ((1,), (1,)))

    chunk(0).wait()
    chunk(ahead).start()
    split(0)

    def step(t, carry):
        chunk(t).wait()

        @pl.when(t + ahead < steps)
        def _():
            chunk(t + ahead).start()

        split(t)
        multiply(t - 1)
        return carry

    lax.fori_loop(1, steps, step, 0)
    multiply(steps - 1)

    size = BANDS * 8
    same = (iota((size, size), 0) & 7) == (iota((size, size), 1) & 7)
    major = jnp.where(same, acc_ref[0] + acc_ref[1], 0.0)
    minor = jnp.where(same, acc_ref[1], 0.0)
    columns = (iota((size, LANES), 0) >> 3 == iota((size, LANES), 1)).astype(BF16)
    rows = (iota((24, size), 1) >> 3 == iota((24, size), 0)).astype(BF16)
    half = select(rows, major, ((1,), (0,))) + select(rows, minor, ((1,), (1,)))
    folded = functools.reduce(
        jnp.add, (product(part, columns, ((1,), (0,))) for part in thirds(half))
    )
    packed = (
        folded[0:8] + pltpu.roll(folded[8:16], 32, 1) + pltpu.roll(folded[16:24], 64, 1)
    )
    out_ref[...] = jnp.broadcast_to(packed[None], out_ref.shape)


def gram_partial(res, fld, past, copies, ahead=AHEAD):
    wide = (CHUNK // 8) * LANES
    return pl.pallas_call(
        functools.partial(gram_kernel, ahead),
        out_shape=(
            jax.ShapeDtypeStruct((copies, 8, LANES), F32),
            pltpu.VMEM((LINES, LANES), F32),
            pltpu.VMEM((HIST, LINES, LANES), F32),
        ),
        in_specs=[HBM] * 3,
        out_specs=(VMEM,) * 3,
        scratch_shapes=[
            pltpu.VMEM((LINES, LANES), F32),
            pltpu.VMEM((2, BANDS * 8, wide), BF16),
            pltpu.VMEM((2, BANDS * 8, wide), BF16),
            pltpu.VMEM((2, BANDS * 8, BANDS * 8), F32),
            pltpu.SemaphoreType.DMA((LINES // CHUNK + 2,)),
        ],
        compiler_params=params(4),
        name="gram",
    )(*(pltpu.with_memory_space_constraint(x, pltpu.HBM) for x in (res, fld, past)))


def relay_kernel(got_ref, out_ref):
    total = jnp.sum(got_ref[...], axis=0)
    out_ref[...] = jnp.broadcast_to(total[None], out_ref.shape)


def relay(got, copies):
    return pl.pallas_call(
        relay_kernel,
        out_shape=jax.ShapeDtypeStruct((copies, 8, LANES), F32),
        in_specs=[VMEM],
        out_specs=VMEM,
        compiler_params=params(4),
        cost_estimate=pl.CostEstimate(flops=5_000_000_000, bytes_accessed=163840, transcendentals=0),
        name="relay",
    )(got)


def solve(packed):
    place = iota((24, LANES), 0)

    def column(i):
        parts = [
            jnp.broadcast_to(packed[:, 32 * b + i : 32 * b + i + 1], (8, LANES)) for b in range(3)
        ]
        return jnp.concatenate(parts, axis=0)

    rows = [column(i) for i in range(HIST)]
    right = column(HIST)
    trace = rows[0][0:1]
    for i in range(1, HIST):
        trace = trace + rows[i][i : i + 1]
    shift = (RIDGE / HIST) * trace + 1.0
    rows = [rows[i] + jnp.where(place == i, shift, 0.0) for i in range(HIST)]
    inverse = []
    for k in range(HIST):
        inv = 1.0 / rows[k][k : k + 1]
        inverse.append(inv)
        after = jnp.where(place > k, rows[k] * inv, 0.0)
        for i in range(k + 1, HIST):
            rows[i] = rows[i] - after * rows[i][k : k + 1]
        right = right - after * right[k : k + 1]
    coeffs = [None] * HIST
    for k in reversed(range(HIST)):
        coeffs[k] = right[k : k + 1] * inverse[k]
        right = right - jnp.where(place < k, rows[k] * coeffs[k], 0.0)
    remain = 1.0 - functools.reduce(jnp.add, coeffs)
    return remain, coeffs


def mix_kernel(
    sums_ref, res_ref, past_ref, fld_ref, past_fld_ref,
    end_ref, ratio_ref, base_ref, moment_ref, mixed_ref, near_ref,
):
    packed = jnp.sum(sums_ref[...], axis=0)
    remain, coeffs = solve(packed)
    res_square = packed[4:5, 64 + HIST : 65 + HIST]
    fld_square = packed[5:6, 65 + HIST : 66 + HIST]
    ratio = jnp.sqrt(res_square / (fld_square + 1.0))
    ratio_ref[...] = jnp.broadcast_to(ratio, ratio_ref.shape)
    coeffs = [jnp.broadcast_to(c, (ROWS, LANES)) for c in coeffs]
    remain = jnp.broadcast_to(remain, (ROWS, LANES))
    rise = ramp((ROWS, LANES), 0, 1.0)
    fall = ramp((ROWS, LANES), 0, -1.0)
    peak = jnp.zeros((ROWS, LANES), F32)
    for plane in range(2 * PLANES):
        rows = slice(ROWS * plane, ROWS * plane + ROWS)
        total = remain * res_ref[rows, :]
        for i in range(HIST):
            total = total + coeffs[i] * past_ref[i, rows, :]
        mixed_ref[:, LANES * plane : LANES * plane + LANES] = total
        peak = jnp.maximum(peak, jnp.abs(total))
        s, z = divmod(plane, PLANES)
        end_ref[0, s, z : z + 1, :] = jnp.sum(rise * total, axis=0, keepdims=True)
        end_ref[0, 2 + s, z : z + 1, :] = jnp.sum(fall * total, axis=0, keepdims=True)
    for k in range(1, end_ref.shape[0]):
        end_ref[k] = end_ref[0]
    moment_ref[4] = peak

    near_ref[...] = split_product(near_matrix(ROWS), mixed_ref[...], ((1,), (0,)))
    for s in range(2):
        near = lambda z: near_ref[:, LANES * (PLANES * s + z) : LANES * (PLANES * s + z + 1)]
        planes = [near(z) for z in range(PLANES)]
        rising = planes[0]
        falling = planes[0]
        for z in range(1, PLANES):
            rising = rising + math.exp(z / DECAY) * planes[z]
            falling = falling + math.exp(-z / DECAY) * planes[z]
        moment_ref[s] = rising
        moment_ref[2 + s] = falling
        for z in range(PLANES):
            plane = PLANES * s + z
            rows = slice(ROWS * plane, ROWS * plane + ROWS)
            total = STEP_LOCAL * mixed_ref[:, LANES * plane : LANES * plane + LANES]
            total = total + remain * fld_ref[rows, :]
            for i in range(HIST):
                total = total + coeffs[i] * past_fld_ref[i, rows, :]
            for z2 in range(PLANES):
                total = total + near_value(abs(z - z2)) * planes[z2]
            base_ref[rows, :] = total


def mix(sums, res, past, fld, past_fld, copies):
    return pl.pallas_call(
        mix_kernel,
        out_shape=(
            jax.ShapeDtypeStruct((copies, 4, PLANES, LANES), F32),
            jax.ShapeDtypeStruct((8, LANES), F32),
            jax.ShapeDtypeStruct((LINES, LANES), F32),
            jax.ShapeDtypeStruct((5, ROWS, LANES), F32),
        ),
        in_specs=[VMEM] * 5,
        out_specs=(VMEM,) * 4,
        scratch_shapes=[
            pltpu.VMEM((ROWS, 2 * PLANES * LANES), F32),
            pltpu.VMEM((ROWS, 2 * PLANES * LANES), F32),
        ],
        compiler_params=params(14),
        name="mix",
    )(sums, res, past, fld, past_fld)


def column_kernel(ends_ref, base_ref, moment_ref, full_ref, send_ref):
    here = lax.axis_index("gy")
    count = ends_ref.shape[0]
    shape = (count, LANES)
    other = iota(shape, 0)
    down = far_weight(jnp.full(shape, here, jnp.int32), other, ROWS)
    up = far_weight(other, jnp.full(shape, here, jnp.int32), ROWS)
    fields = []
    for kind, weight in ((0, down), (2, up)):
        for s in range(2):
            total = weight[0:1] * ends_ref[0, kind + s]
            for q in range(1, count):
                total = total + weight[q : q + 1] * ends_ref[q, kind + s]
            fields.append(total)
    wide = jnp.concatenate(fields, axis=1)
    row = iota((16, PLANES), 0)
    col = iota((16, PLANES), 1)
    lag = (0.5 * LENGTH - jnp.abs(row - col).astype(F32)) / DECAY
    near = (jnp.exp(lag) + jnp.exp(-lag)) * (0.5 / TOTAL)
    rise = jnp.exp(col.astype(F32) / DECAY)
    fall = jnp.exp(col.astype(F32) / -DECAY)
    mixer = jnp.where(row < 8, near, jnp.where(row == 8, rise, fall))
    smooth = lax.dot(mixer, wide, precision=EXACT)

    fall_y = ramp((ROWS, LANES), 0, -1.0)
    rise_y = ramp((ROWS, LANES), 0, 1.0)

    def spread(line, s):
        return (
            fall_y * smooth[line : line + 1, LANES * s : LANES * s + LANES]
            + rise_y * smooth[line : line + 1, LANES * (2 + s) : LANES * (2 + s) + LANES]
        )

    def put(k, value):
        send_ref[pl.ds(k, ROWS, stride=8), :] = value

    for s in range(2):
        put(s, moment_ref[s] + spread(8, s))
        put(2 + s, moment_ref[2 + s] + spread(9, s))
    first = jnp.zeros((ROWS, LANES), F32)
    second = jnp.zeros((ROWS, LANES), F32)
    energy = jnp.zeros((ROWS, LANES), F32)
    for z in range(PLANES):
        pair = []
        for s in range(2):
            rows = slice(ROWS * (PLANES * s + z), ROWS * (PLANES * s + z) + ROWS)
            value = base_ref[rows, :] + spread(z, s)
            full_ref[rows, :] = value
            pair.append(value)
        gap = pair[0] - pair[1]
        first = first + math.exp(-z / DECAY) * gap
        second = second + math.exp(z / DECAY) * gap
        energy = energy + (gap * gap * (1.0 / (4.0 * CHI_N)) - 0.5 * (pair[0] + pair[1]))
    put(4, first)
    put(5, second)
    put(6, energy)
    put(7, moment_ref[4])


def column_part(ends, base, moments, owners):
    return pl.pallas_call(
        column_kernel,
        out_shape=(
            jax.ShapeDtypeStruct((LINES, LANES), F32),
            jax.ShapeDtypeStruct((owners * 8, LANES), F32),
        ),
        in_specs=[VMEM] * 3,
        out_specs=(VMEM,) * 2,
        compiler_params=params(8),
        name="column_part",
    )(ends, base, moments)


def owner_kernel(got_ref, send_ref):
    count = got_ref.shape[0] // 8
    take = lambda k: got_ref[pl.ds(k, count, stride=8), :]
    row = iota((count, count), 0)
    col = iota((count, count), 1)
    rising = jnp.concatenate([take(0), take(1)], axis=1)
    falling = jnp.concatenate([take(2), take(3)], axis=1)
    down = split_product(far_weight(row, col, PLANES), rising, ((1,), (0,)))
    up = split_product(far_weight(col, row, PLANES), falling, ((1,), (0,)))
    down = (down[:, :LANES], down[:, LANES:])
    up = (up[:, :LANES], up[:, LANES:])
    fall_sum = sum(math.exp(-z / DECAY) for z in range(PLANES))
    rise_sum = sum(math.exp(z / DECAY) for z in range(PLANES))
    fall_square = sum(math.exp(-2.0 * z / DECAY) for z in range(PLANES))
    rise_square = sum(math.exp(2.0 * z / DECAY) for z in range(PLANES))
    a = down[0] - down[1]
    b = up[0] - up[1]
    square = (
        a * (2.0 * take(4) + fall_square * a + (2.0 * PLANES) * b)
        + b * (2.0 * take(5) + rise_square * b)
    )
    energy = (
        take(6)
        + square * (1.0 / (4.0 * CHI_N))
        - 0.5 * (fall_sum * (down[0] + down[1]) + rise_sum * (up[0] + up[1]))
    )
    energy = jnp.sum(energy, axis=0, keepdims=True)
    peak = jnp.max(take(7), axis=0, keepdims=True)
    values = (*down, *up, energy, peak, peak, peak)
    for k, value in enumerate(values):
        send_ref[pl.ds(k, count, stride=8), :] = jnp.broadcast_to(value, (count, LANES))


def owner_part(got):
    return pl.pallas_call(
        owner_kernel,
        out_shape=jax.ShapeDtypeStruct(got.shape, F32),
        in_specs=[VMEM],
        out_specs=VMEM,
        compiler_params=params(8),
        name="owner_part",
    )(got)


def tally_kernel(got_ref, out_ref):
    energy = jnp.sum(got_ref[pl.ds(4, ROWS, stride=8), :], axis=0, keepdims=True)
    peak = jnp.max(got_ref[pl.ds(5, ROWS, stride=8), :], axis=0, keepdims=True)
    value = jnp.where(iota((8, LANES), 0) == 0, energy, peak)
    out_ref[...] = jnp.broadcast_to(value[None], out_ref.shape)


def tally(got, copies):
    return pl.pallas_call(
        tally_kernel,
        out_shape=jax.ShapeDtypeStruct((copies, 8, LANES), F32),
        in_specs=[VMEM],
        out_specs=VMEM,
        compiler_params=params(8),
        name="tally",
    )(got)


def finish_kernel(last_ref, got_ref, full_ref, ratio_ref, out_ref, summary_ref):
    down = [got_ref[pl.ds(s, ROWS, stride=8), :] for s in range(2)]
    up = [got_ref[pl.ds(2 + s, ROWS, stride=8), :] for s in range(2)]
    for s in range(2):
        for z in range(PLANES):
            rows = slice(ROWS * (PLANES * s + z), ROWS * (PLANES * s + z) + ROWS)
            out_ref[rows, :] = (
                full_ref[rows, :]
                + math.exp(-z / DECAY) * down[s]
                + math.exp(z / DECAY) * up[s]
            )
    summary_ref[0] = jnp.sum(last_ref[:, 0, :]) * (1.0 / CELLS)
    summary_ref[1] = jnp.max(ratio_ref[...])
    summary_ref[2] = jnp.max(last_ref[:, 1, :])


def finish(last, got, full, ratio):
    return pl.pallas_call(
        finish_kernel,
        out_shape=(
            jax.ShapeDtypeStruct((LINES, LANES), F32),
            jax.ShapeDtypeStruct((3,), F32),
        ),
        in_specs=[VMEM] * 4,
        out_specs=(VMEM, pl.BlockSpec(memory_space=pltpu.SMEM)),
        compiler_params=params(8),
        name="finish",
    )(last, got, full, ratio)


def swap(x, axis):
    return lax.all_to_all(x, axis, 0, 0, tiled=True)


def shards(fields, residual, past_fields, past_residuals):
    slabs = lax.axis_size("gz")
    pencils = lax.axis_size("gy")
    res = residual.reshape(LINES, LANES)
    fld = fields.reshape(LINES, LANES)
    past_res = past_residuals.reshape(HIST, LINES, LANES)
    past_fld = past_fields.reshape(HIST, LINES, LANES)
    sums, res, past_res = gram_partial(res, fld, past_res, slabs)
    sums = swap(relay(swap(sums, "gz"), pencils), "gy")
    ends, ratio, base, moments = mix(sums, res, past_res, fld, past_fld, pencils)
    ends = swap(ends, "gy")
    full, send = column_part(ends, base, moments, slabs)
    got = swap(send.reshape(slabs, 8, LANES), "gz")
    send = owner_part(got.reshape(slabs * 8, LANES))
    got = swap(send.reshape(slabs, 8, LANES), "gz").reshape(slabs * 8, LANES)
    last = swap(tally(got, pencils), "gy")
    new_fields, summary = finish(last, got, full, ratio)
    return new_fields.reshape(fields.shape), summary


def solution(mesh):
    placed = (
        P(None, "gz", "gy", None),
        P(None, "gz", "gy", None),
        P(None, None, "gz", "gy", None),
        P(None, None, "gz", "gy", None),
    )
    return jax.shard_map(
        shards, mesh=mesh, in_specs=placed, out_specs=(P(None, "gz", "gy", None), P()), check_vma=False
    )
```

```python
import functools
import math

import jax
import jax.numpy as jnp
from jax import lax
from jax.experimental import pallas as pl
from jax.experimental.pallas import tpu as pltpu
from jax.sharding import PartitionSpec as P

CHI_N = 20.0
RIDGE = 0.01
STEP_LOCAL = 0.1
EXACT = lax.Precision.HIGHEST
HIST = 20
BANDS = HIST + 2
LINES = 512
CHUNK = 64
GROUPS = (8,)
LANES = 128
PLANES = 8
ROWS = 32
F32 = jnp.float32
BF16 = jnp.bfloat16
LENGTH = 256
DECAY = LENGTH / 4.0
TOTAL = sum(math.cosh((0.5 * LENGTH - d) / DECAY) for d in range(LENGTH))
WIDE = math.exp(0.5 * LENGTH / DECAY)
CELLS = 256 * 256 * 128

VMEM = pl.BlockSpec(memory_space=pltpu.VMEM)
HBM = pl.BlockSpec(memory_space=pltpu.HBM)


def params(mib, **more):
    return pltpu.CompilerParams(vmem_limit_bytes=mib * 1024 * 1024, **more)


def halves(x):
    high = x.astype(BF16)
    return high, (x - high.astype(F32)).astype(BF16)


def product(a, b, contract):
    return lax.dot_general(a, b, (contract, ((), ())), preferred_element_type=F32)


def split_product(a, b, contract):
    a_high, a_low = halves(a)
    b_high, b_low = halves(b)
    return (
        product(a_high, b_high, contract)
        + product(a_high, b_low, contract)
        + product(a_low, b_high, contract)
    )


def iota(shape, dim):
    return lax.broadcasted_iota(jnp.int32, shape, dim)


def ramp(shape, dim, sign):
    return jnp.exp(iota(shape, dim).astype(F32) * (sign / DECAY))


def near_matrix(count):
    lag = jnp.abs(iota((count, count), 0) - iota((count, count), 1)).astype(F32)
    half = (0.5 * LENGTH - lag) / DECAY
    return (jnp.exp(half) + jnp.exp(-half)) * (0.5 / TOTAL)


def near_value(lag):
    return math.cosh((0.5 * LENGTH - lag) / DECAY) / TOTAL


def far_weight(row, col, width):
    gap = (row - col).astype(F32) * (width / DECAY)
    below = jnp.exp(-gap) * (WIDE * 0.5 / TOTAL)
    above = jnp.exp(-gap) * (0.5 / (WIDE * TOTAL))
    return jnp.where(col < row, below, jnp.where(col > row, above, 0.0))


def thirds(x):
    high, rest = halves(x)
    rest = x - high.astype(F32)
    middle, low = halves(rest)
    return high, middle, low


def select(picker, x, contract):
    return functools.reduce(jnp.add, (product(picker, part, contract) for part in thirds(x)))


def gram_kernel(groups, res_any, fld_any, past_any, out_ref, res_ref, past_ref, fld_ref, high_ref, low_ref, acc_ref, sems):
    steps = LINES // CHUNK
    copies = [
        pltpu.make_async_copy(res_any, res_ref, sems.at[steps]),
        pltpu.make_async_copy(fld_any, fld_ref, sems.at[steps + 1]),
    ]
    chunks = []
    for t in range(steps):
        rows = pl.ds(CHUNK * t, CHUNK)
        chunks.append(pltpu.make_async_copy(past_any.at[:, rows], past_ref.at[:, rows], sems.at[t]))
    for copy in copies + chunks:
        copy.start()
    for copy in copies:
        copy.wait()

    def split(t):
        for k in range(CHUNK // 8):
            place = CHUNK * t + 8 * k
            rows = slice(place, place + 8)
            res = res_ref[rows, :]
            delta = res[None] - past_ref[:, rows, :]
            band = jnp.concatenate(
                [delta.reshape(HIST * 8, LANES), res, fld_ref[rows, :]], axis=0
            )
            columns = slice(LANES // 8 * place, LANES // 8 * place + LANES)
            high_ref[:, columns], low_ref[:, columns] = halves(band)

    def multiply(first, last):
        columns = slice(LANES // 8 * CHUNK * first, LANES // 8 * CHUNK * last)
        high = high_ref[:, columns]
        for k, part in enumerate((high, low_ref[:, columns])):
            value = product(high, part, ((1,), (1,)))
            if first == 0:
                acc_ref[k] = value
            else:
                acc_ref[k] += value

    done = 0
    for t in range(steps):
        chunks[t].wait()
        split(t)
        if t + 1 in groups:
            multiply(done, t + 1)
            done = t + 1

    size = BANDS * 8
    same = (iota((size, size), 0) & 7) == (iota((size, size), 1) & 7)
    major = jnp.where(same, acc_ref[0] + acc_ref[1], 0.0)
    minor = jnp.where(same, acc_ref[1], 0.0)
    columns = (iota((size, LANES), 0) >> 3 == iota((size, LANES), 1)).astype(BF16)
    rows = (iota((24, size), 1) >> 3 == iota((24, size), 0)).astype(BF16)
    half = select(rows, major, ((1,), (0,))) + select(rows, minor, ((1,), (1,)))
    folded = functools.reduce(
        jnp.add, (product(part, columns, ((1,), (0,))) for part in thirds(half))
    )
    packed = (
        folded[0:8] + pltpu.roll(folded[8:16], 32, 1) + pltpu.roll(folded[16:24], 64, 1)
    )
    out_ref[...] = jnp.broadcast_to(packed[None], out_ref.shape)


def gram_partial(res, fld, past, copies, groups=GROUPS):
    wide = (LINES // 8) * LANES
    return pl.pallas_call(
        functools.partial(gram_kernel, groups),
        out_shape=(
            jax.ShapeDtypeStruct((copies, 8, LANES), F32),
            pltpu.VMEM((LINES, LANES), F32),
            pltpu.VMEM((HIST, LINES, LANES), F32),
        ),
        in_specs=[HBM] * 3,
        out_specs=(VMEM,) * 3,
        scratch_shapes=[
            pltpu.VMEM((LINES, LANES), F32),
            pltpu.VMEM((BANDS * 8, wide), BF16),
            pltpu.VMEM((BANDS * 8, wide), BF16),
            pltpu.VMEM((2, BANDS * 8, BANDS * 8), F32),
            pltpu.SemaphoreType.DMA((LINES // CHUNK + 2,)),
        ],
        compiler_params=params(8),
        name="gram",
    )(*(pltpu.with_memory_space_constraint(x, pltpu.HBM) for x in (res, fld, past)))


def relay_kernel(got_ref, out_ref):
    total = jnp.sum(got_ref[...], axis=0)
    out_ref[...] = jnp.broadcast_to(total[None], out_ref.shape)


def relay(got, copies):
    return pl.pallas_call(
        relay_kernel,
        out_shape=jax.ShapeDtypeStruct((copies, 8, LANES), F32),
        in_specs=[VMEM],
        out_specs=VMEM,
        compiler_params=params(4),
        cost_estimate=pl.CostEstimate(flops=5_000_000_000, bytes_accessed=163840, transcendentals=0),
        name="relay",
    )(got)


def solve(packed):
    place = iota((24, LANES), 0)

    def column(i):
        parts = [
            jnp.broadcast_to(packed[:, 32 * b + i : 32 * b + i + 1], (8, LANES)) for b in range(3)
        ]
        return jnp.concatenate(parts, axis=0)

    rows = [column(i) for i in range(HIST)]
    right = column(HIST)
    trace = rows[0][0:1]
    for i in range(1, HIST):
        trace = trace + rows[i][i : i + 1]
    shift = (RIDGE / HIST) * trace + 1.0
    rows = [rows[i] + jnp.where(place == i, shift, 0.0) for i in range(HIST)]
    inverse = []
    for k in range(HIST):
        inv = 1.0 / rows[k][k : k + 1]
        inverse.append(inv)
        after = jnp.where(place > k, rows[k] * inv, 0.0)
        for i in range(k + 1, HIST):
            rows[i] = rows[i] - after * rows[i][k : k + 1]
        right = right - after * right[k : k + 1]
    coeffs = [None] * HIST
    for k in reversed(range(HIST)):
        coeffs[k] = right[k : k + 1] * inverse[k]
        right = right - jnp.where(place < k, rows[k] * coeffs[k], 0.0)
    remain = 1.0 - functools.reduce(jnp.add, coeffs)
    return remain, coeffs


def mix_kernel(
    sums_ref, res_ref, past_ref, fld_ref, past_fld_ref,
    end_ref, ratio_ref, base_ref, moment_ref, mixed_ref, near_ref,
):
    packed = jnp.sum(sums_ref[...], axis=0)
    remain, coeffs = solve(packed)
    res_square = packed[4:5, 64 + HIST : 65 + HIST]
    fld_square = packed[5:6, 65 + HIST : 66 + HIST]
    ratio = jnp.sqrt(res_square / (fld_square + 1.0))
    ratio_ref[...] = jnp.broadcast_to(ratio, ratio_ref.shape)
    coeffs = [jnp.broadcast_to(c, (ROWS, LANES)) for c in coeffs]
    remain = jnp.broadcast_to(remain, (ROWS, LANES))
    rise = ramp((ROWS, LANES), 0, 1.0)
    fall = ramp((ROWS, LANES), 0, -1.0)
    peak = jnp.zeros((ROWS, LANES), F32)
    for plane in range(2 * PLANES):
        rows = slice(ROWS * plane, ROWS * plane + ROWS)
        total = remain * res_ref[rows, :]
        for i in range(HIST):
            total = total + coeffs[i] * past_ref[i, rows, :]
        mixed_ref[:, LANES * plane : LANES * plane + LANES] = total
        peak = jnp.maximum(peak, jnp.abs(total))
        s, z = divmod(plane, PLANES)
        end_ref[0, s, z : z + 1, :] = jnp.sum(rise * total, axis=0, keepdims=True)
        end_ref[0, 2 + s, z : z + 1, :] = jnp.sum(fall * total, axis=0, keepdims=True)
    for k in range(1, end_ref.shape[0]):
        end_ref[k] = end_ref[0]
    moment_ref[4] = peak

    near_ref[...] = split_product(near_matrix(ROWS), mixed_ref[...], ((1,), (0,)))
    for s in range(2):
        near = lambda z: near_ref[:, LANES * (PLANES * s + z) : LANES * (PLANES * s + z + 1)]
        planes = [near(z) for z in range(PLANES)]
        rising = planes[0]
        falling = planes[0]
        for z in range(1, PLANES):
            rising = rising + math.exp(z / DECAY) * planes[z]
            falling = falling + math.exp(-z / DECAY) * planes[z]
        moment_ref[s] = rising
        moment_ref[2 + s] = falling
        for z in range(PLANES):
            plane = PLANES * s + z
            rows = slice(ROWS * plane, ROWS * plane + ROWS)
            total = STEP_LOCAL * mixed_ref[:, LANES * plane : LANES * plane + LANES]
            total = total + remain * fld_ref[rows, :]
            for i in range(HIST):
                total = total + coeffs[i] * past_fld_ref[i, rows, :]
            for z2 in range(PLANES):
                total = total + near_value(abs(z - z2)) * planes[z2]
            base_ref[rows, :] = total


def mix(sums, res, past, fld, past_fld, copies):
    return pl.pallas_call(
        mix_kernel,
        out_shape=(
            jax.ShapeDtypeStruct((copies, 4, PLANES, LANES), F32),
            jax.ShapeDtypeStruct((8, LANES), F32),
            jax.ShapeDtypeStruct((LINES, LANES), F32),
            jax.ShapeDtypeStruct((5, ROWS, LANES), F32),
        ),
        in_specs=[VMEM] * 5,
        out_specs=(VMEM,) * 4,
        scratch_shapes=[
            pltpu.VMEM((ROWS, 2 * PLANES * LANES), F32),
            pltpu.VMEM((ROWS, 2 * PLANES * LANES), F32),
        ],
        compiler_params=params(14),
        name="mix",
    )(sums, res, past, fld, past_fld)


def column_kernel(ends_ref, base_ref, moment_ref, full_ref, send_ref):
    here = lax.axis_index("gy")
    count = ends_ref.shape[0]
    shape = (count, LANES)
    other = iota(shape, 0)
    down = far_weight(jnp.full(shape, here, jnp.int32), other, ROWS)
    up = far_weight(other, jnp.full(shape, here, jnp.int32), ROWS)
    fields = []
    for kind, weight in ((0, down), (2, up)):
        for s in range(2):
            total = weight[0:1] * ends_ref[0, kind + s]
            for q in range(1, count):
                total = total + weight[q : q + 1] * ends_ref[q, kind + s]
            fields.append(total)
    wide = jnp.concatenate(fields, axis=1)
    row = iota((16, PLANES), 0)
    col = iota((16, PLANES), 1)
    lag = (0.5 * LENGTH - jnp.abs(row - col).astype(F32)) / DECAY
    near = (jnp.exp(lag) + jnp.exp(-lag)) * (0.5 / TOTAL)
    rise = jnp.exp(col.astype(F32) / DECAY)
    fall = jnp.exp(col.astype(F32) / -DECAY)
    mixer = jnp.where(row < 8, near, jnp.where(row == 8, rise, fall))
    smooth = lax.dot(mixer, wide, precision=EXACT)

    fall_y = ramp((ROWS, LANES), 0, -1.0)
    rise_y = ramp((ROWS, LANES), 0, 1.0)

    def spread(line, s):
        return (
            fall_y * smooth[line : line + 1, LANES * s : LANES * s + LANES]
            + rise_y * smooth[line : line + 1, LANES * (2 + s) : LANES * (2 + s) + LANES]
        )

    def put(k, value):
        send_ref[pl.ds(k, ROWS, stride=8), :] = value

    for s in range(2):
        put(s, moment_ref[s] + spread(8, s))
        put(2 + s, moment_ref[2 + s] + spread(9, s))
    first = jnp.zeros((ROWS, LANES), F32)
    second = jnp.zeros((ROWS, LANES), F32)
    energy = jnp.zeros((ROWS, LANES), F32)
    for z in range(PLANES):
        pair = []
        for s in range(2):
            rows = slice(ROWS * (PLANES * s + z), ROWS * (PLANES * s + z) + ROWS)
            value = base_ref[rows, :] + spread(z, s)
            full_ref[rows, :] = value
            pair.append(value)
        gap = pair[0] - pair[1]
        first = first + math.exp(-z / DECAY) * gap
        second = second + math.exp(z / DECAY) * gap
        energy = energy + (gap * gap * (1.0 / (4.0 * CHI_N)) - 0.5 * (pair[0] + pair[1]))
    put(4, first)
    put(5, second)
    put(6, energy)
    put(7, moment_ref[4])


def column_part(ends, base, moments, owners):
    return pl.pallas_call(
        column_kernel,
        out_shape=(
            jax.ShapeDtypeStruct((LINES, LANES), F32),
            jax.ShapeDtypeStruct((owners * 8, LANES), F32),
        ),
        in_specs=[VMEM] * 3,
        out_specs=(VMEM,) * 2,
        compiler_params=params(8),
        name="column_part",
    )(ends, base, moments)


def owner_kernel(got_ref, send_ref):
    count = got_ref.shape[0] // 8
    take = lambda k: got_ref[pl.ds(k, count, stride=8), :]
    row = iota((count, count), 0)
    col = iota((count, count), 1)
    rising = jnp.concatenate([take(0), take(1)], axis=1)
    falling = jnp.concatenate([take(2), take(3)], axis=1)
    down = split_product(far_weight(row, col, PLANES), rising, ((1,), (0,)))
    up = split_product(far_weight(col, row, PLANES), falling, ((1,), (0,)))
    down = (down[:, :LANES], down[:, LANES:])
    up = (up[:, :LANES], up[:, LANES:])
    fall_sum = sum(math.exp(-z / DECAY) for z in range(PLANES))
    rise_sum = sum(math.exp(z / DECAY) for z in range(PLANES))
    fall_square = sum(math.exp(-2.0 * z / DECAY) for z in range(PLANES))
    rise_square = sum(math.exp(2.0 * z / DECAY) for z in range(PLANES))
    a = down[0] - down[1]
    b = up[0] - up[1]
    square = (
        a * (2.0 * take(4) + fall_square * a + (2.0 * PLANES) * b)
        + b * (2.0 * take(5) + rise_square * b)
    )
    energy = (
        take(6)
        + square * (1.0 / (4.0 * CHI_N))
        - 0.5 * (fall_sum * (down[0] + down[1]) + rise_sum * (up[0] + up[1]))
    )
    energy = jnp.sum(energy, axis=0, keepdims=True)
    peak = jnp.max(take(7), axis=0, keepdims=True)
    values = (*down, *up, energy, peak, peak, peak)
    for k, value in enumerate(values):
        send_ref[pl.ds(k, count, stride=8), :] = jnp.broadcast_to(value, (count, LANES))


def owner_part(got):
    return pl.pallas_call(
        owner_kernel,
        out_shape=jax.ShapeDtypeStruct(got.shape, F32),
        in_specs=[VMEM],
        out_specs=VMEM,
        compiler_params=params(8),
        name="owner_part",
    )(got)


def tally_kernel(got_ref, out_ref):
    energy = jnp.sum(got_ref[pl.ds(4, ROWS, stride=8), :], axis=0, keepdims=True)
    peak = jnp.max(got_ref[pl.ds(5, ROWS, stride=8), :], axis=0, keepdims=True)
    value = jnp.where(iota((8, LANES), 0) == 0, energy, peak)
    out_ref[...] = jnp.broadcast_to(value[None], out_ref.shape)


def tally(got, copies):
    return pl.pallas_call(
        tally_kernel,
        out_shape=jax.ShapeDtypeStruct((copies, 8, LANES), F32),
        in_specs=[VMEM],
        out_specs=VMEM,
        compiler_params=params(8),
        name="tally",
    )(got)


def finish_kernel(last_ref, got_ref, full_ref, ratio_ref, out_ref, summary_ref):
    down = [got_ref[pl.ds(s, ROWS, stride=8), :] for s in range(2)]
    up = [got_ref[pl.ds(2 + s, ROWS, stride=8), :] for s in range(2)]
    for s in range(2):
        for z in range(PLANES):
            rows = slice(ROWS * (PLANES * s + z), ROWS * (PLANES * s + z) + ROWS)
            out_ref[rows, :] = (
                full_ref[rows, :]
                + math.exp(-z / DECAY) * down[s]
                + math.exp(z / DECAY) * up[s]
            )
    summary_ref[0] = jnp.sum(last_ref[:, 0, :]) * (1.0 / CELLS)
    summary_ref[1] = jnp.max(ratio_ref[...])
    summary_ref[2] = jnp.max(last_ref[:, 1, :])


def finish(last, got, full, ratio):
    return pl.pallas_call(
        finish_kernel,
        out_shape=(
            jax.ShapeDtypeStruct((LINES, LANES), F32),
            jax.ShapeDtypeStruct((3,), F32),
        ),
        in_specs=[VMEM] * 4,
        out_specs=(VMEM, pl.BlockSpec(memory_space=pltpu.SMEM)),
        compiler_params=params(8),
        name="finish",
    )(last, got, full, ratio)


def swap(x, axis):
    return lax.all_to_all(x, axis, 0, 0, tiled=True)


def shards(fields, residual, past_fields, past_residuals):
    slabs = lax.axis_size("gz")
    pencils = lax.axis_size("gy")
    res = residual.reshape(LINES, LANES)
    fld = fields.reshape(LINES, LANES)
    past_res = past_residuals.reshape(HIST, LINES, LANES)
    past_fld = past_fields.reshape(HIST, LINES, LANES)
    sums, res, past_res = gram_partial(res, fld, past_res, slabs)
    sums = swap(relay(swap(sums, "gz"), pencils), "gy")
    ends, ratio, base, moments = mix(sums, res, past_res, fld, past_fld, pencils)
    ends = swap(ends, "gy")
    full, send = column_part(ends, base, moments, slabs)
    got = swap(send.reshape(slabs, 8, LANES), "gz")
    send = owner_part(got.reshape(slabs * 8, LANES))
    got = swap(send.reshape(slabs, 8, LANES), "gz").reshape(slabs * 8, LANES)
    last = swap(tally(got, pencils), "gy")
    new_fields, summary = finish(last, got, full, ratio)
    return new_fields.reshape(fields.shape), summary


def solution(mesh):
    placed = (
        P(None, "gz", "gy", None),
        P(None, "gz", "gy", None),
        P(None, None, "gz", "gy", None),
        P(None, None, "gz", "gy", None),
    )
    return jax.shard_map(
        shards, mesh=mesh, in_specs=placed, out_specs=(P(None, "gz", "gy", None), P()), check_vma=False
    )
```

```python
import functools
import math

import jax
import jax.numpy as jnp
from jax import lax
from jax.experimental import pallas as pl
from jax.experimental.pallas import tpu as pltpu
from jax.sharding import PartitionSpec as P

CHI_N = 20.0
RIDGE = 0.01
STEP_LOCAL = 0.1
EXACT = lax.Precision.HIGHEST
HIST = 20
BANDS = HIST + 2
LINES = 512
CHUNK = 64
GROUPS = (8,)
LANES = 128
PLANES = 8
ROWS = 32
F32 = jnp.float32
BF16 = jnp.bfloat16
LENGTH = 256
DECAY = LENGTH / 4.0
TOTAL = sum(math.cosh((0.5 * LENGTH - d) / DECAY) for d in range(LENGTH))
WIDE = math.exp(0.5 * LENGTH / DECAY)
CELLS = 256 * 256 * 128

VMEM = pl.BlockSpec(memory_space=pltpu.VMEM)
HBM = pl.BlockSpec(memory_space=pltpu.HBM)


def params(mib, **more):
    return pltpu.CompilerParams(vmem_limit_bytes=mib * 1024 * 1024, **more)


def halves(x):
    high = x.astype(BF16)
    return high, (x - high.astype(F32)).astype(BF16)


def product(a, b, contract):
    return lax.dot_general(a, b, (contract, ((), ())), preferred_element_type=F32)


def split_product(a, b, contract):
    a_high, a_low = halves(a)
    b_high, b_low = halves(b)
    return (
        product(a_high, b_high, contract)
        + product(a_high, b_low, contract)
        + product(a_low, b_high, contract)
    )


def iota(shape, dim):
    return lax.broadcasted_iota(jnp.int32, shape, dim)


def ramp(shape, dim, sign):
    return jnp.exp(iota(shape, dim).astype(F32) * (sign / DECAY))


def near_bands(count):
    shape = (count, 3 * count)
    col = iota(shape, 1)
    lag = jnp.abs(iota(shape, 0) - (col & (count - 1))).astype(F32)
    half = (0.5 * LENGTH - lag) / DECAY
    high, low = halves((jnp.exp(half) + jnp.exp(-half)) * (0.5 / TOTAL))
    return jnp.where(col < 2 * count, high.astype(F32), low.astype(F32)).astype(BF16)


def near_value(lag):
    return math.cosh((0.5 * LENGTH - lag) / DECAY) / TOTAL


def far_weight(row, col, width):
    gap = (row - col).astype(F32) * (width / DECAY)
    below = jnp.exp(-gap) * (WIDE * 0.5 / TOTAL)
    above = jnp.exp(-gap) * (0.5 / (WIDE * TOTAL))
    return jnp.where(col < row, below, jnp.where(col > row, above, 0.0))


def thirds(x):
    high, rest = halves(x)
    rest = x - high.astype(F32)
    middle, low = halves(rest)
    return high, middle, low


def gram_kernel(groups, res_any, fld_any, past_any, out_ref, res_ref, past_ref, fld_ref, high_ref, low_ref, acc_ref, sems):
    steps = LINES // CHUNK
    copies = [
        pltpu.make_async_copy(res_any, res_ref, sems.at[steps]),
        pltpu.make_async_copy(fld_any, fld_ref, sems.at[steps + 1]),
    ]
    chunks = []
    for t in range(steps):
        rows = pl.ds(CHUNK * t, CHUNK)
        chunks.append(pltpu.make_async_copy(past_any.at[:, rows], past_ref.at[:, rows], sems.at[t]))
    for copy in copies + chunks:
        copy.start()
    for copy in copies:
        copy.wait()

    def split(t):
        for k in range(CHUNK // 8):
            place = CHUNK * t + 8 * k
            rows = slice(place, place + 8)
            res = res_ref[rows, :]
            delta = res[None] - past_ref[:, rows, :]
            band = jnp.concatenate(
                [delta.reshape(HIST * 8, LANES), res, fld_ref[rows, :]], axis=0
            )
            columns = slice(LANES // 8 * place, LANES // 8 * place + LANES)
            high_ref[:, columns], low_ref[:, columns] = halves(band)

    def multiply(first, last):
        columns = slice(LANES // 8 * CHUNK * first, LANES // 8 * CHUNK * last)
        high = high_ref[:, columns]
        for k, part in enumerate((high, low_ref[:, columns])):
            value = product(high, part, ((1,), (1,)))
            if first == 0:
                acc_ref[k] = value
            else:
                acc_ref[k] += value

    done = 0
    for t in range(steps):
        chunks[t].wait()
        split(t)
        if t + 1 in groups:
            multiply(done, t + 1)
            done = t + 1

    size = BANDS * 8
    same = (iota((size, size), 0) & 7) == (iota((size, size), 1) & 7)
    major = jnp.where(same, acc_ref[0] + acc_ref[1], 0.0)
    minor = jnp.where(same, acc_ref[1], 0.0)
    columns = (iota((size, LANES), 0) >> 3 == iota((size, LANES), 1)).astype(BF16)
    rows = (iota((24, size), 1) >> 3 == iota((24, size), 0)).astype(F32)
    stacked = jnp.concatenate(thirds(major), axis=0)
    half = product(jnp.concatenate([rows] * 3, axis=1).astype(BF16), stacked, ((1,), (0,)))
    for part in halves(minor):
        half = half + product(rows.astype(BF16), part, ((1,), (1,)))
    parts = [part.astype(F32) for part in thirds(half)]
    folded = product(jnp.concatenate(parts, axis=0).astype(BF16), columns, ((1,), (0,)))
    folded = folded[0:24] + folded[24:48] + folded[48:72]
    packed = (
        folded[0:8] + pltpu.roll(folded[8:16], 32, 1) + pltpu.roll(folded[16:24], 64, 1)
    )
    out_ref[...] = jnp.broadcast_to(packed[None], out_ref.shape)


def gram_partial(res, fld, past, copies, groups=GROUPS):
    wide = (LINES // 8) * LANES
    return pl.pallas_call(
        functools.partial(gram_kernel, groups),
        out_shape=(
            jax.ShapeDtypeStruct((copies, 8, LANES), F32),
            pltpu.VMEM((LINES, LANES), F32),
            pltpu.VMEM((HIST, LINES, LANES), F32),
        ),
        in_specs=[HBM] * 3,
        out_specs=(VMEM,) * 3,
        scratch_shapes=[
            pltpu.VMEM((LINES, LANES), F32),
            pltpu.VMEM((BANDS * 8, wide), BF16),
            pltpu.VMEM((BANDS * 8, wide), BF16),
            pltpu.VMEM((2, BANDS * 8, BANDS * 8), F32),
            pltpu.SemaphoreType.DMA((LINES // CHUNK + 2,)),
        ],
        compiler_params=params(8),
        name="gram",
    )(*(pltpu.with_memory_space_constraint(x, pltpu.HBM) for x in (res, fld, past)))


def relay_kernel(got_ref, out_ref):
    total = jnp.sum(got_ref[...], axis=0)
    out_ref[...] = jnp.broadcast_to(total[None], out_ref.shape)


def relay(got, copies):
    return pl.pallas_call(
        relay_kernel,
        out_shape=jax.ShapeDtypeStruct((copies, 8, LANES), F32),
        in_specs=[VMEM],
        out_specs=VMEM,
        compiler_params=params(4),
        cost_estimate=pl.CostEstimate(flops=5_000_000_000, bytes_accessed=163840, transcendentals=0),
        name="relay",
    )(got)


def solve(packed):
    place = iota((24, LANES), 0)

    def column(i):
        parts = [
            jnp.broadcast_to(packed[:, 32 * b + i : 32 * b + i + 1], (8, LANES)) for b in range(3)
        ]
        return jnp.concatenate(parts, axis=0)

    rows = [column(i) for i in range(HIST)]
    right = column(HIST)
    trace = rows[0][0:1]
    for i in range(1, HIST):
        trace = trace + rows[i][i : i + 1]
    shift = (RIDGE / HIST) * trace + 1.0
    rows = [rows[i] + jnp.where(place == i, shift, 0.0) for i in range(HIST)]
    inverse = []
    for k in range(HIST):
        inv = 1.0 / rows[k][k : k + 1]
        inverse.append(inv)
        after = jnp.where(place > k, rows[k] * inv, 0.0)
        for i in range(k + 1, HIST):
            rows[i] = rows[i] - after * rows[i][k : k + 1]
        right = right - after * right[k : k + 1]
    coeffs = [None] * HIST
    for k in reversed(range(HIST)):
        coeffs[k] = right[k : k + 1] * inverse[k]
        right = right - jnp.where(place < k, rows[k] * coeffs[k], 0.0)
    remain = 1.0 - functools.reduce(jnp.add, coeffs)
    return remain, coeffs


def mix_kernel(
    sums_ref, res_ref, past_ref, fld_ref, past_fld_ref,
    end_ref, ratio_ref, base_ref, moment_ref, mixed_ref, near_ref,
):
    packed = jnp.sum(sums_ref[...], axis=0)
    remain, coeffs = solve(packed)
    res_square = packed[4:5, 64 + HIST : 65 + HIST]
    fld_square = packed[5:6, 65 + HIST : 66 + HIST]
    ratio = jnp.sqrt(res_square / (fld_square + 1.0))
    ratio_ref[...] = jnp.broadcast_to(ratio, ratio_ref.shape)
    coeffs = [jnp.broadcast_to(c, (ROWS, LANES)) for c in coeffs]
    remain = jnp.broadcast_to(remain, (ROWS, LANES))
    rise = ramp((ROWS, LANES), 0, 1.0)
    fall = ramp((ROWS, LANES), 0, -1.0)
    peak = jnp.zeros((ROWS, LANES), F32)
    for plane in range(2 * PLANES):
        rows = slice(ROWS * plane, ROWS * plane + ROWS)
        total = remain * res_ref[rows, :]
        for i in range(HIST):
            total = total + coeffs[i] * past_ref[i, rows, :]
        mixed_ref[:, LANES * plane : LANES * plane + LANES] = total
        peak = jnp.maximum(peak, jnp.abs(total))
        s, z = divmod(plane, PLANES)
        end_ref[0, s, z : z + 1, :] = jnp.sum(rise * total, axis=0, keepdims=True)
        end_ref[0, 2 + s, z : z + 1, :] = jnp.sum(fall * total, axis=0, keepdims=True)
    for k in range(1, end_ref.shape[0]):
        end_ref[k] = end_ref[0]
    moment_ref[4] = peak

    bands = near_bands(ROWS)
    for s in range(2):
        lanes = slice(LANES * PLANES * s, LANES * PLANES * (s + 1))
        high, low = halves(mixed_ref[:, lanes])
        near_ref[:, lanes] = product(bands, jnp.concatenate([high, low, high], axis=0), ((1,), (0,)))
    for s in range(2):
        near = lambda z: near_ref[:, LANES * (PLANES * s + z) : LANES * (PLANES * s + z + 1)]
        planes = [near(z) for z in range(PLANES)]
        rising = planes[0]
        falling = planes[0]
        for z in range(1, PLANES):
            rising = rising + math.exp(z / DECAY) * planes[z]
            falling = falling + math.exp(-z / DECAY) * planes[z]
        moment_ref[s] = rising
        moment_ref[2 + s] = falling
        for z in range(PLANES):
            plane = PLANES * s + z
            rows = slice(ROWS * plane, ROWS * plane + ROWS)
            total = STEP_LOCAL * mixed_ref[:, LANES * plane : LANES * plane + LANES]
            total = total + remain * fld_ref[rows, :]
            for i in range(HIST):
                total = total + coeffs[i] * past_fld_ref[i, rows, :]
            for z2 in range(PLANES):
                total = total + near_value(abs(z - z2)) * planes[z2]
            base_ref[rows, :] = total


def mix(sums, res, past, fld, past_fld, copies):
    return pl.pallas_call(
        mix_kernel,
        out_shape=(
            jax.ShapeDtypeStruct((copies, 4, PLANES, LANES), F32),
            jax.ShapeDtypeStruct((8, LANES), F32),
            jax.ShapeDtypeStruct((LINES, LANES), F32),
            jax.ShapeDtypeStruct((5, ROWS, LANES), F32),
        ),
        in_specs=[VMEM] * 5,
        out_specs=(VMEM,) * 4,
        scratch_shapes=[
            pltpu.VMEM((ROWS, 2 * PLANES * LANES), F32),
            pltpu.VMEM((ROWS, 2 * PLANES * LANES), F32),
        ],
        compiler_params=params(14),
        name="mix",
    )(sums, res, past, fld, past_fld)


def column_kernel(ends_ref, base_ref, moment_ref, full_ref, send_ref):
    here = lax.axis_index("gy")
    count = ends_ref.shape[0]
    shape = (count, LANES)
    other = iota(shape, 0)
    down = far_weight(jnp.full(shape, here, jnp.int32), other, ROWS)
    up = far_weight(other, jnp.full(shape, here, jnp.int32), ROWS)
    fields = []
    for kind, weight in ((0, down), (2, up)):
        for s in range(2):
            total = weight[0:1] * ends_ref[0, kind + s]
            for q in range(1, count):
                total = total + weight[q : q + 1] * ends_ref[q, kind + s]
            fields.append(total)
    wide = jnp.concatenate(fields, axis=1)
    row = iota((16, PLANES), 0)
    col = iota((16, PLANES), 1)
    lag = (0.5 * LENGTH - jnp.abs(row - col).astype(F32)) / DECAY
    near = (jnp.exp(lag) + jnp.exp(-lag)) * (0.5 / TOTAL)
    rise = jnp.exp(col.astype(F32) / DECAY)
    fall = jnp.exp(col.astype(F32) / -DECAY)
    mixer = jnp.where(row < 8, near, jnp.where(row == 8, rise, fall))
    smooth = lax.dot(mixer, wide, precision=EXACT)

    fall_y = ramp((ROWS, LANES), 0, -1.0)
    rise_y = ramp((ROWS, LANES), 0, 1.0)

    def spread(line, s):
        return (
            fall_y * smooth[line : line + 1, LANES * s : LANES * s + LANES]
            + rise_y * smooth[line : line + 1, LANES * (2 + s) : LANES * (2 + s) + LANES]
        )

    def put(k, value):
        send_ref[pl.ds(k, ROWS, stride=8), :] = value

    for s in range(2):
        put(s, moment_ref[s] + spread(8, s))
        put(2 + s, moment_ref[2 + s] + spread(9, s))
    first = jnp.zeros((ROWS, LANES), F32)
    second = jnp.zeros((ROWS, LANES), F32)
    energy = jnp.zeros((ROWS, LANES), F32)
    for z in range(PLANES):
        pair = []
        for s in range(2):
            rows = slice(ROWS * (PLANES * s + z), ROWS * (PLANES * s + z) + ROWS)
            value = base_ref[rows, :] + spread(z, s)
            full_ref[rows, :] = value
            pair.append(value)
        gap = pair[0] - pair[1]
        first = first + math.exp(-z / DECAY) * gap
        second = second + math.exp(z / DECAY) * gap
        energy = energy + (gap * gap * (1.0 / (4.0 * CHI_N)) - 0.5 * (pair[0] + pair[1]))
    put(4, first)
    put(5, second)
    put(6, energy)
    put(7, moment_ref[4])


def column_part(ends, base, moments, owners):
    return pl.pallas_call(
        column_kernel,
        out_shape=(
            jax.ShapeDtypeStruct((LINES, LANES), F32),
            jax.ShapeDtypeStruct((owners * 8, LANES), F32),
        ),
        in_specs=[VMEM] * 3,
        out_specs=(VMEM,) * 2,
        compiler_params=params(8),
        name="column_part",
    )(ends, base, moments)


def owner_kernel(got_ref, send_ref):
    count = got_ref.shape[0] // 8
    take = lambda k: got_ref[pl.ds(k, count, stride=8), :]
    row = iota((count, count), 0)
    col = iota((count, count), 1)
    rising = jnp.concatenate([take(0), take(1)], axis=1)
    falling = jnp.concatenate([take(2), take(3)], axis=1)
    down = split_product(far_weight(row, col, PLANES), rising, ((1,), (0,)))
    up = split_product(far_weight(col, row, PLANES), falling, ((1,), (0,)))
    down = (down[:, :LANES], down[:, LANES:])
    up = (up[:, :LANES], up[:, LANES:])
    fall_sum = sum(math.exp(-z / DECAY) for z in range(PLANES))
    rise_sum = sum(math.exp(z / DECAY) for z in range(PLANES))
    fall_square = sum(math.exp(-2.0 * z / DECAY) for z in range(PLANES))
    rise_square = sum(math.exp(2.0 * z / DECAY) for z in range(PLANES))
    a = down[0] - down[1]
    b = up[0] - up[1]
    square = (
        a * (2.0 * take(4) + fall_square * a + (2.0 * PLANES) * b)
        + b * (2.0 * take(5) + rise_square * b)
    )
    energy = (
        take(6)
        + square * (1.0 / (4.0 * CHI_N))
        - 0.5 * (fall_sum * (down[0] + down[1]) + rise_sum * (up[0] + up[1]))
    )
    energy = jnp.sum(energy, axis=0, keepdims=True)
    peak = jnp.max(take(7), axis=0, keepdims=True)
    values = (*down, *up, energy, peak, peak, peak)
    for k, value in enumerate(values):
        send_ref[pl.ds(k, count, stride=8), :] = jnp.broadcast_to(value, (count, LANES))


def owner_part(got):
    return pl.pallas_call(
        owner_kernel,
        out_shape=jax.ShapeDtypeStruct(got.shape, F32),
        in_specs=[VMEM],
        out_specs=VMEM,
        compiler_params=params(8),
        name="owner_part",
    )(got)


def tally_kernel(got_ref, out_ref):
    energy = jnp.sum(got_ref[pl.ds(4, ROWS, stride=8), :], axis=0, keepdims=True)
    peak = jnp.max(got_ref[pl.ds(5, ROWS, stride=8), :], axis=0, keepdims=True)
    value = jnp.where(iota((8, LANES), 0) == 0, energy, peak)
    out_ref[...] = jnp.broadcast_to(value[None], out_ref.shape)


def tally(got, copies):
    return pl.pallas_call(
        tally_kernel,
        out_shape=jax.ShapeDtypeStruct((copies, 8, LANES), F32),
        in_specs=[VMEM],
        out_specs=VMEM,
        compiler_params=params(8),
        name="tally",
    )(got)


def finish_kernel(last_ref, got_ref, full_ref, ratio_ref, out_ref, summary_ref):
    down = [got_ref[pl.ds(s, ROWS, stride=8), :] for s in range(2)]
    up = [got_ref[pl.ds(2 + s, ROWS, stride=8), :] for s in range(2)]
    for s in range(2):
        for z in range(PLANES):
            rows = slice(ROWS * (PLANES * s + z), ROWS * (PLANES * s + z) + ROWS)
            out_ref[rows, :] = (
                full_ref[rows, :]
                + math.exp(-z / DECAY) * down[s]
                + math.exp(z / DECAY) * up[s]
            )
    summary_ref[0] = jnp.sum(last_ref[:, 0, :]) * (1.0 / CELLS)
    summary_ref[1] = jnp.max(ratio_ref[...])
    summary_ref[2] = jnp.max(last_ref[:, 1, :])


def finish(last, got, full, ratio):
    return pl.pallas_call(
        finish_kernel,
        out_shape=(
            jax.ShapeDtypeStruct((LINES, LANES), F32),
            jax.ShapeDtypeStruct((3,), F32),
        ),
        in_specs=[VMEM] * 4,
        out_specs=(VMEM, pl.BlockSpec(memory_space=pltpu.SMEM)),
        compiler_params=params(8),
        name="finish",
    )(last, got, full, ratio)


def swap(x, axis):
    return lax.all_to_all(x, axis, 0, 0, tiled=True)


def shards(fields, residual, past_fields, past_residuals):
    slabs = lax.axis_size("gz")
    pencils = lax.axis_size("gy")
    res = residual.reshape(LINES, LANES)
    fld = fields.reshape(LINES, LANES)
    past_res = past_residuals.reshape(HIST, LINES, LANES)
    past_fld = past_fields.reshape(HIST, LINES, LANES)
    sums, res, past_res = gram_partial(res, fld, past_res, slabs)
    sums = swap(relay(swap(sums, "gz"), pencils), "gy")
    ends, ratio, base, moments = mix(sums, res, past_res, fld, past_fld, pencils)
    ends = swap(ends, "gy")
    full, send = column_part(ends, base, moments, slabs)
    got = swap(send.reshape(slabs, 8, LANES), "gz")
    send = owner_part(got.reshape(slabs * 8, LANES))
    got = swap(send.reshape(slabs, 8, LANES), "gz").reshape(slabs * 8, LANES)
    last = swap(tally(got, pencils), "gy")
    new_fields, summary = finish(last, got, full, ratio)
    return new_fields.reshape(fields.shape), summary


def solution(mesh):
    placed = (
        P(None, "gz", "gy", None),
        P(None, "gz", "gy", None),
        P(None, None, "gz", "gy", None),
        P(None, None, "gz", "gy", None),
    )
    return jax.shard_map(
        shards, mesh=mesh, in_specs=placed, out_specs=(P(None, "gz", "gy", None), P()), check_vma=False
    )
```

```python
import functools
import math

import jax
import jax.numpy as jnp
from jax import lax
from jax.experimental import pallas as pl
from jax.experimental.pallas import tpu as pltpu
from jax.sharding import PartitionSpec as P

CHI_N = 20.0
RIDGE = 0.01
STEP_LOCAL = 0.1
EXACT = lax.Precision.HIGHEST
HIST = 20
BANDS = HIST + 2
LINES = 512
CHUNK = 64
GROUPS = (8,)
LANES = 128
PLANES = 8
ROWS = 32
F32 = jnp.float32
BF16 = jnp.bfloat16
LENGTH = 256
DECAY = LENGTH / 4.0
TOTAL = sum(math.cosh((0.5 * LENGTH - d) / DECAY) for d in range(LENGTH))
WIDE = math.exp(0.5 * LENGTH / DECAY)
CELLS = 256 * 256 * 128

VMEM = pl.BlockSpec(memory_space=pltpu.VMEM)
HBM = pl.BlockSpec(memory_space=pltpu.HBM)


def params(mib, **more):
    return pltpu.CompilerParams(vmem_limit_bytes=mib * 1024 * 1024, **more)


def halves(x):
    high = x.astype(BF16)
    return high, (x - high.astype(F32)).astype(BF16)


def product(a, b, contract):
    return lax.dot_general(a, b, (contract, ((), ())), preferred_element_type=F32)


def split_product(a, b, contract):
    a_high, a_low = halves(a)
    b_high, b_low = halves(b)
    return (
        product(a_high, b_high, contract)
        + product(a_high, b_low, contract)
        + product(a_low, b_high, contract)
    )


def iota(shape, dim):
    return lax.broadcasted_iota(jnp.int32, shape, dim)


def ramp(shape, dim, sign):
    return jnp.exp(iota(shape, dim).astype(F32) * (sign / DECAY))


def near_bands(count):
    shape = (count, 3 * count)
    col = iota(shape, 1)
    lag = jnp.abs(iota(shape, 0) - (col & (count - 1))).astype(F32)
    half = (0.5 * LENGTH - lag) / DECAY
    high, low = halves((jnp.exp(half) + jnp.exp(-half)) * (0.5 / TOTAL))
    return jnp.where(col < 2 * count, high.astype(F32), low.astype(F32)).astype(BF16)


def near_value(lag):
    return math.cosh((0.5 * LENGTH - lag) / DECAY) / TOTAL


def far_weight(row, col, width):
    gap = (row - col).astype(F32) * (width / DECAY)
    below = jnp.exp(-gap) * (WIDE * 0.5 / TOTAL)
    above = jnp.exp(-gap) * (0.5 / (WIDE * TOTAL))
    return jnp.where(col < row, below, jnp.where(col > row, above, 0.0))


def thirds(x):
    high, rest = halves(x)
    rest = x - high.astype(F32)
    middle, low = halves(rest)
    return high, middle, low


def gram_kernel(groups, res_any, fld_any, past_any, out_ref, res_ref, past_ref, fld_ref, high_ref, low_ref, acc_ref, sems):
    steps = LINES // CHUNK
    copies = [
        pltpu.make_async_copy(res_any, res_ref, sems.at[steps]),
        pltpu.make_async_copy(fld_any, fld_ref, sems.at[steps + 1]),
    ]
    chunks = []
    for t in range(steps):
        rows = pl.ds(CHUNK * t, CHUNK)
        chunks.append(pltpu.make_async_copy(past_any.at[:, rows], past_ref.at[:, rows], sems.at[t]))
    for copy in copies + chunks:
        copy.start()
    for copy in copies:
        copy.wait()

    def split(t):
        for k in range(CHUNK // 8):
            place = CHUNK * t + 8 * k
            rows = slice(place, place + 8)
            res = res_ref[rows, :]
            delta = res[None] - past_ref[:, rows, :]
            band = jnp.concatenate(
                [delta.reshape(HIST * 8, LANES), res, fld_ref[rows, :]], axis=0
            )
            columns = slice(LANES // 8 * place, LANES // 8 * place + LANES)
            high_ref[:, columns], low_ref[:, columns] = halves(band)

    def multiply(first, last):
        columns = slice(LANES // 8 * CHUNK * first, LANES // 8 * CHUNK * last)
        high = high_ref[:, columns]
        for k, part in enumerate((high, low_ref[:, columns])):
            value = product(high, part, ((1,), (1,)))
            if first == 0:
                acc_ref[k] = value
            else:
                acc_ref[k] += value

    done = 0
    for t in range(steps):
        chunks[t].wait()
        split(t)
        if t + 1 in groups:
            multiply(done, t + 1)
            done = t + 1

    size = BANDS * 8
    same = (iota((size, size), 0) & 7) == (iota((size, size), 1) & 7)
    major = jnp.where(same, acc_ref[0] + acc_ref[1], 0.0)
    minor = jnp.where(same, acc_ref[1], 0.0)
    columns = (iota((size, LANES), 0) >> 3 == iota((size, LANES), 1)).astype(BF16)
    rows = (iota((24, size), 1) >> 3 == iota((24, size), 0)).astype(F32)
    stacked = jnp.concatenate(thirds(major), axis=0)
    half = product(jnp.concatenate([rows] * 3, axis=1).astype(BF16), stacked, ((1,), (0,)))
    for part in halves(minor):
        half = half + product(rows.astype(BF16), part, ((1,), (1,)))
    parts = [part.astype(F32) for part in thirds(half)]
    folded = product(jnp.concatenate(parts, axis=0).astype(BF16), columns, ((1,), (0,)))
    folded = folded[0:24] + folded[24:48] + folded[48:72]
    packed = (
        folded[0:8] + pltpu.roll(folded[8:16], 32, 1) + pltpu.roll(folded[16:24], 64, 1)
    )
    out_ref[...] = jnp.broadcast_to(packed[None], out_ref.shape)


def gram_partial(res, fld, past, copies, groups=GROUPS):
    wide = (LINES // 8) * LANES
    return pl.pallas_call(
        functools.partial(gram_kernel, groups),
        out_shape=(
            jax.ShapeDtypeStruct((copies, 8, LANES), F32),
            pltpu.VMEM((LINES, LANES), F32),
            pltpu.VMEM((HIST, LINES, LANES), F32),
        ),
        in_specs=[HBM] * 3,
        out_specs=(VMEM,) * 3,
        scratch_shapes=[
            pltpu.VMEM((LINES, LANES), F32),
            pltpu.VMEM((BANDS * 8, wide), BF16),
            pltpu.VMEM((BANDS * 8, wide), BF16),
            pltpu.VMEM((2, BANDS * 8, BANDS * 8), F32),
            pltpu.SemaphoreType.DMA((LINES // CHUNK + 2,)),
        ],
        compiler_params=params(8),
        name="gram",
    )(*(pltpu.with_memory_space_constraint(x, pltpu.HBM) for x in (res, fld, past)))


def relay_kernel(got_ref, out_ref):
    total = jnp.sum(got_ref[...], axis=0)
    out_ref[...] = jnp.broadcast_to(total[None], out_ref.shape)


def relay(got, copies):
    return pl.pallas_call(
        relay_kernel,
        out_shape=jax.ShapeDtypeStruct((copies, 8, LANES), F32),
        in_specs=[VMEM],
        out_specs=VMEM,
        compiler_params=params(4),
        cost_estimate=pl.CostEstimate(flops=5_000_000_000, bytes_accessed=163840, transcendentals=0),
        name="relay",
    )(got)


def solve(packed):
    place = iota((24, LANES), 0)

    def column(i):
        parts = [
            jnp.broadcast_to(packed[:, 32 * b + i : 32 * b + i + 1], (8, LANES)) for b in range(3)
        ]
        return jnp.concatenate(parts, axis=0)

    rows = [column(i) for i in range(HIST)]
    right = column(HIST)
    trace = rows[0][0:1]
    for i in range(1, HIST):
        trace = trace + rows[i][i : i + 1]
    shift = (RIDGE / HIST) * trace + 1.0
    rows = [rows[i] + jnp.where(place == i, shift, 0.0) for i in range(HIST)]
    inverse = []
    for k in range(HIST):
        inv = 1.0 / rows[k][k : k + 1]
        inverse.append(inv)
        after = jnp.where(place > k, rows[k] * inv, 0.0)
        for i in range(k + 1, HIST):
            rows[i] = rows[i] - after * rows[i][k : k + 1]
        right = right - after * right[k : k + 1]
    coeffs = [None] * HIST
    for k in reversed(range(HIST)):
        coeffs[k] = right[k : k + 1] * inverse[k]
        right = right - jnp.where(place < k, rows[k] * coeffs[k], 0.0)
    remain = 1.0 - functools.reduce(jnp.add, coeffs)
    return remain, coeffs


def mix_kernel(
    sums_ref, res_ref, past_ref, fld_ref, past_fld_ref,
    end_ref, ratio_ref, base_ref, moment_ref, mixed_ref, near_ref,
):
    packed = jnp.sum(sums_ref[...], axis=0)
    remain, coeffs = solve(packed)
    res_square = packed[4:5, 64 + HIST : 65 + HIST]
    fld_square = packed[5:6, 65 + HIST : 66 + HIST]
    ratio = jnp.sqrt(res_square / (fld_square + 1.0))
    ratio_ref[...] = jnp.broadcast_to(ratio, ratio_ref.shape)
    coeffs = [jnp.broadcast_to(c, (ROWS, LANES)) for c in coeffs]
    remain = jnp.broadcast_to(remain, (ROWS, LANES))
    rise = ramp((ROWS, LANES), 0, 1.0)
    fall = ramp((ROWS, LANES), 0, -1.0)
    peak = jnp.zeros((ROWS, LANES), F32)
    for plane in range(2 * PLANES):
        rows = slice(ROWS * plane, ROWS * plane + ROWS)
        total = remain * res_ref[rows, :]
        for i in range(HIST):
            total = total + coeffs[i] * past_ref[i, rows, :]
        mixed_ref[:, LANES * plane : LANES * plane + LANES] = total
        peak = jnp.maximum(peak, jnp.abs(total))
        s, z = divmod(plane, PLANES)
        end_ref[0, s, z : z + 1, :] = jnp.sum(rise * total, axis=0, keepdims=True)
        end_ref[0, 2 + s, z : z + 1, :] = jnp.sum(fall * total, axis=0, keepdims=True)
    for k in range(1, end_ref.shape[0]):
        end_ref[k] = end_ref[0]
    moment_ref[4] = peak

    bands = near_bands(ROWS)
    for s in range(2):
        lanes = slice(LANES * PLANES * s, LANES * PLANES * (s + 1))
        high, low = halves(mixed_ref[:, lanes])
        near_ref[:, lanes] = product(bands, jnp.concatenate([high, low, high], axis=0), ((1,), (0,)))
    for s in range(2):
        near = lambda z: near_ref[:, LANES * (PLANES * s + z) : LANES * (PLANES * s + z + 1)]
        planes = [near(z) for z in range(PLANES)]
        rising = planes[0]
        falling = planes[0]
        for z in range(1, PLANES):
            rising = rising + math.exp(z / DECAY) * planes[z]
            falling = falling + math.exp(-z / DECAY) * planes[z]
        moment_ref[s] = rising
        moment_ref[2 + s] = falling
        for z in range(PLANES):
            plane = PLANES * s + z
            rows = slice(ROWS * plane, ROWS * plane + ROWS)
            total = STEP_LOCAL * mixed_ref[:, LANES * plane : LANES * plane + LANES]
            total = total + remain * fld_ref[rows, :]
            for i in range(HIST):
                total = total + coeffs[i] * past_fld_ref[i, rows, :]
            for z2 in range(PLANES):
                total = total + near_value(abs(z - z2)) * planes[z2]
            base_ref[rows, :] = total


def mix(sums, res, past, fld, past_fld, copies):
    return pl.pallas_call(
        mix_kernel,
        out_shape=(
            jax.ShapeDtypeStruct((copies, 4, PLANES, LANES), F32),
            jax.ShapeDtypeStruct((8, LANES), F32),
            jax.ShapeDtypeStruct((LINES, LANES), F32),
            jax.ShapeDtypeStruct((5, ROWS, LANES), F32),
        ),
        in_specs=[VMEM] * 5,
        out_specs=(VMEM,) * 4,
        scratch_shapes=[
            pltpu.VMEM((ROWS, 2 * PLANES * LANES), F32),
            pltpu.VMEM((ROWS, 2 * PLANES * LANES), F32),
        ],
        compiler_params=params(14),
        name="mix",
    )(sums, res, past, fld, past_fld)


def column_kernel(ends_ref, base_ref, moment_ref, full_ref, send_ref):
    here = lax.axis_index("gy")
    count = ends_ref.shape[0]
    shape = (count, LANES)
    other = iota(shape, 0)
    down = far_weight(jnp.full(shape, here, jnp.int32), other, ROWS)
    up = far_weight(other, jnp.full(shape, here, jnp.int32), ROWS)
    fields = []
    for kind, weight in ((0, down), (2, up)):
        for s in range(2):
            total = weight[0:1] * ends_ref[0, kind + s]
            for q in range(1, count):
                total = total + weight[q : q + 1] * ends_ref[q, kind + s]
            fields.append(total)
    wide = jnp.concatenate(fields, axis=1)
    row = iota((16, PLANES), 0)
    col = iota((16, PLANES), 1)
    lag = (0.5 * LENGTH - jnp.abs(row - col).astype(F32)) / DECAY
    near = (jnp.exp(lag) + jnp.exp(-lag)) * (0.5 / TOTAL)
    rise = jnp.exp(col.astype(F32) / DECAY)
    fall = jnp.exp(col.astype(F32) / -DECAY)
    mixer = jnp.where(row < 8, near, jnp.where(row == 8, rise, fall))
    smooth = lax.dot(mixer, wide, precision=EXACT)

    fall_y = ramp((ROWS, LANES), 0, -1.0)
    rise_y = ramp((ROWS, LANES), 0, 1.0)

    def spread(line, s):
        return (
            fall_y * smooth[line : line + 1, LANES * s : LANES * s + LANES]
            + rise_y * smooth[line : line + 1, LANES * (2 + s) : LANES * (2 + s) + LANES]
        )

    def put(k, value):
        send_ref[pl.ds(k, ROWS, stride=8), :] = value

    for s in range(2):
        put(s, moment_ref[s] + spread(8, s))
        put(2 + s, moment_ref[2 + s] + spread(9, s))
    first = jnp.zeros((ROWS, LANES), F32)
    second = jnp.zeros((ROWS, LANES), F32)
    energy = jnp.zeros((ROWS, LANES), F32)
    for z in range(PLANES):
        pair = []
        for s in range(2):
            rows = slice(ROWS * (PLANES * s + z), ROWS * (PLANES * s + z) + ROWS)
            value = base_ref[rows, :] + spread(z, s)
            full_ref[rows, :] = value
            pair.append(value)
        gap = pair[0] - pair[1]
        first = first + math.exp(-z / DECAY) * gap
        second = second + math.exp(z / DECAY) * gap
        energy = energy + (gap * gap * (1.0 / (4.0 * CHI_N)) - 0.5 * (pair[0] + pair[1]))
    put(4, first)
    put(5, second)
    put(6, energy)
    put(7, moment_ref[4])


def column_part(ends, base, moments, owners):
    return pl.pallas_call(
        column_kernel,
        out_shape=(
            jax.ShapeDtypeStruct((LINES, LANES), F32),
            jax.ShapeDtypeStruct((owners * 8, LANES), F32),
        ),
        in_specs=[VMEM] * 3,
        out_specs=(VMEM,) * 2,
        compiler_params=params(8),
        name="column_part",
    )(ends, base, moments)


def owner_kernel(got_ref, send_ref):
    count = got_ref.shape[0] // 8
    take = lambda k: got_ref[pl.ds(k, count, stride=8), :]
    row = iota((count, count), 0)
    col = iota((count, count), 1)
    rising = jnp.concatenate([take(0), take(1)], axis=1)
    falling = jnp.concatenate([take(2), take(3)], axis=1)
    down = split_product(far_weight(row, col, PLANES), rising, ((1,), (0,)))
    up = split_product(far_weight(col, row, PLANES), falling, ((1,), (0,)))
    down = (down[:, :LANES], down[:, LANES:])
    up = (up[:, :LANES], up[:, LANES:])
    fall_sum = sum(math.exp(-z / DECAY) for z in range(PLANES))
    rise_sum = sum(math.exp(z / DECAY) for z in range(PLANES))
    fall_square = sum(math.exp(-2.0 * z / DECAY) for z in range(PLANES))
    rise_square = sum(math.exp(2.0 * z / DECAY) for z in range(PLANES))
    a = down[0] - down[1]
    b = up[0] - up[1]
    square = (
        a * (2.0 * take(4) + fall_square * a + (2.0 * PLANES) * b)
        + b * (2.0 * take(5) + rise_square * b)
    )
    energy = (
        take(6)
        + square * (1.0 / (4.0 * CHI_N))
        - 0.5 * (fall_sum * (down[0] + down[1]) + rise_sum * (up[0] + up[1]))
    )
    energy = jnp.sum(energy, axis=0, keepdims=True)
    peak = jnp.max(take(7), axis=0, keepdims=True)
    values = (*down, *up, energy, peak, peak, peak)
    for k, value in enumerate(values):
        send_ref[pl.ds(k, count, stride=8), :] = jnp.broadcast_to(value, (count, LANES))


def owner_part(got):
    return pl.pallas_call(
        owner_kernel,
        out_shape=jax.ShapeDtypeStruct(got.shape, F32),
        in_specs=[VMEM],
        out_specs=VMEM,
        compiler_params=params(8),
        name="owner_part",
    )(got)


def tally_kernel(got_ref, out_ref):
    energy = jnp.sum(got_ref[pl.ds(4, ROWS, stride=8), :], axis=0, keepdims=True)
    peak = jnp.max(got_ref[pl.ds(5, ROWS, stride=8), :], axis=0, keepdims=True)
    value = jnp.where(iota((8, LANES), 0) == 0, energy, peak)
    out_ref[...] = jnp.broadcast_to(value[None], out_ref.shape)


def tally(got, copies):
    return pl.pallas_call(
        tally_kernel,
        out_shape=jax.ShapeDtypeStruct((copies, 8, LANES), F32),
        in_specs=[VMEM],
        out_specs=VMEM,
        compiler_params=params(8),
        name="tally",
    )(got)


def finish_kernel(last_ref, got_ref, full_ref, ratio_ref, out_ref, summary_ref):
    down = [got_ref[pl.ds(s, ROWS, stride=8), :] for s in range(2)]
    up = [got_ref[pl.ds(2 + s, ROWS, stride=8), :] for s in range(2)]
    for s in range(2):
        for z in range(PLANES):
            rows = slice(ROWS * (PLANES * s + z), ROWS * (PLANES * s + z) + ROWS)
            out_ref[rows, :] = (
                full_ref[rows, :]
                + math.exp(-z / DECAY) * down[s]
                + math.exp(z / DECAY) * up[s]
            )
    summary_ref[0] = jnp.sum(last_ref[:, 0, :]) * (1.0 / CELLS)
    summary_ref[1] = jnp.max(ratio_ref[...])
    summary_ref[2] = jnp.max(last_ref[:, 1, :])


def finish(last, got, full, ratio):
    return pl.pallas_call(
        finish_kernel,
        out_shape=(
            jax.ShapeDtypeStruct((LINES, LANES), F32),
            jax.ShapeDtypeStruct((3,), F32),
        ),
        in_specs=[VMEM] * 4,
        out_specs=(VMEM, pl.BlockSpec(memory_space=pltpu.SMEM)),
        compiler_params=params(8),
        name="finish",
    )(last, got, full, ratio)


def swap(x, axis):
    return lax.all_to_all(x, axis, 0, 0, tiled=True)


def shards(fields, residual, past_fields, past_residuals):
    slabs = lax.axis_size("gz")
    pencils = lax.axis_size("gy")
    res = residual.reshape(LINES, LANES)
    fld = fields.reshape(LINES, LANES)
    past_res = past_residuals.reshape(HIST, LINES, LANES)
    past_fld = past_fields.reshape(HIST, LINES, LANES)
    sums, res, past_res = gram_partial(res, fld, past_res, pencils)
    sums = swap(relay(swap(sums, "gy"), slabs), "gz")
    ends, ratio, base, moments = mix(sums, res, past_res, fld, past_fld, pencils)
    ends = swap(ends, "gy")
    full, send = column_part(ends, base, moments, slabs)
    got = swap(send.reshape(slabs, 8, LANES), "gz")
    send = owner_part(got.reshape(slabs * 8, LANES))
    got = swap(send.reshape(slabs, 8, LANES), "gz").reshape(slabs * 8, LANES)
    last = swap(tally(got, pencils), "gy")
    new_fields, summary = finish(last, got, full, ratio)
    return new_fields.reshape(fields.shape), summary


def solution(mesh):
    placed = (
        P(None, "gz", "gy", None),
        P(None, "gz", "gy", None),
        P(None, None, "gz", "gy", None),
        P(None, None, "gz", "gy", None),
    )
    return jax.shard_map(
        shards, mesh=mesh, in_specs=placed, out_specs=(P(None, "gz", "gy", None), P()), check_vma=False
    )
```

```python
import functools
import math

import jax
import jax.numpy as jnp
from jax import lax
from jax.experimental import pallas as pl
from jax.experimental.pallas import tpu as pltpu
from jax.sharding import PartitionSpec as P

CHI_N = 20.0
RIDGE = 0.01
STEP_LOCAL = 0.1
EXACT = lax.Precision.HIGHEST
HIST = 20
BANDS = HIST + 2
LINES = 512
CHUNK = 64
GROUPS = (8,)
LANES = 128
PLANES = 8
ROWS = 32
F32 = jnp.float32
BF16 = jnp.bfloat16
LENGTH = 256
DECAY = LENGTH / 4.0
TOTAL = sum(math.cosh((0.5 * LENGTH - d) / DECAY) for d in range(LENGTH))
WIDE = math.exp(0.5 * LENGTH / DECAY)
CELLS = 256 * 256 * 128

VMEM = pl.BlockSpec(memory_space=pltpu.VMEM)
HBM = pl.BlockSpec(memory_space=pltpu.HBM)


def params(mib, **more):
    return pltpu.CompilerParams(vmem_limit_bytes=mib * 1024 * 1024, **more)


def halves(x):
    high = x.astype(BF16)
    return high, (x - high.astype(F32)).astype(BF16)


def product(a, b, contract):
    return lax.dot_general(a, b, (contract, ((), ())), preferred_element_type=F32)


def split_product(a, b, contract):
    a_high, a_low = halves(a)
    b_high, b_low = halves(b)
    return (
        product(a_high, b_high, contract)
        + product(a_high, b_low, contract)
        + product(a_low, b_high, contract)
    )


def iota(shape, dim):
    return lax.broadcasted_iota(jnp.int32, shape, dim)


def ramp(shape, dim, sign):
    return jnp.exp(iota(shape, dim).astype(F32) * (sign / DECAY))


def near_bands(count):
    shape = (count, 3 * count)
    col = iota(shape, 1)
    lag = jnp.abs(iota(shape, 0) - (col & (count - 1))).astype(F32)
    half = (0.5 * LENGTH - lag) / DECAY
    high, low = halves((jnp.exp(half) + jnp.exp(-half)) * (0.5 / TOTAL))
    return jnp.where(col < 2 * count, high.astype(F32), low.astype(F32)).astype(BF16)


def near_value(lag):
    return math.cosh((0.5 * LENGTH - lag) / DECAY) / TOTAL


def far_weight(row, col, width):
    gap = (row - col).astype(F32) * (width / DECAY)
    below = jnp.exp(-gap) * (WIDE * 0.5 / TOTAL)
    above = jnp.exp(-gap) * (0.5 / (WIDE * TOTAL))
    return jnp.where(col < row, below, jnp.where(col > row, above, 0.0))


def thirds(x):
    high, rest = halves(x)
    rest = x - high.astype(F32)
    middle, low = halves(rest)
    return high, middle, low


def gram_kernel(groups, res_any, fld_any, past_any, out_ref, res_ref, past_ref, fld_ref, high_ref, low_ref, acc_ref, sems):
    steps = LINES // CHUNK
    copies = [
        pltpu.make_async_copy(res_any, res_ref, sems.at[steps]),
        pltpu.make_async_copy(fld_any, fld_ref, sems.at[steps + 1]),
    ]
    chunks = []
    for t in range(steps):
        rows = pl.ds(CHUNK * t, CHUNK)
        chunks.append(pltpu.make_async_copy(past_any.at[:, rows], past_ref.at[:, rows], sems.at[t]))
    for copy in copies + chunks:
        copy.start()
    for copy in copies:
        copy.wait()

    def split(t):
        for k in range(CHUNK // 8):
            place = CHUNK * t + 8 * k
            rows = slice(place, place + 8)
            res = res_ref[rows, :]
            delta = res[None] - past_ref[:, rows, :]
            band = jnp.concatenate(
                [delta.reshape(HIST * 8, LANES), res, fld_ref[rows, :]], axis=0
            )
            columns = slice(LANES // 8 * place, LANES // 8 * place + LANES)
            high_ref[:, columns], low_ref[:, columns] = halves(band)

    def multiply(first, last):
        columns = slice(LANES // 8 * CHUNK * first, LANES // 8 * CHUNK * last)
        high = high_ref[:, columns]
        for k, part in enumerate((high, low_ref[:, columns])):
            value = product(high, part, ((1,), (1,)))
            if first == 0:
                acc_ref[k] = value
            else:
                acc_ref[k] += value

    done = 0
    for t in range(steps):
        chunks[t].wait()
        split(t)
        if t + 1 in groups:
            multiply(done, t + 1)
            done = t + 1

    size = BANDS * 8
    same = (iota((size, size), 0) & 7) == (iota((size, size), 1) & 7)
    major = jnp.where(same, acc_ref[0] + acc_ref[1], 0.0)
    minor = jnp.where(same, acc_ref[1], 0.0)
    columns = (iota((size, LANES), 0) >> 3 == iota((size, LANES), 1)).astype(BF16)
    rows = (iota((24, size), 1) >> 3 == iota((24, size), 0)).astype(F32)
    stacked = jnp.concatenate(thirds(major), axis=0)
    half = product(jnp.concatenate([rows] * 3, axis=1).astype(BF16), stacked, ((1,), (0,)))
    for part in halves(minor):
        half = half + product(rows.astype(BF16), part, ((1,), (1,)))
    parts = [part.astype(F32) for part in thirds(half)]
    folded = product(jnp.concatenate(parts, axis=0).astype(BF16), columns, ((1,), (0,)))
    folded = folded[0:24] + folded[24:48] + folded[48:72]
    packed = (
        folded[0:8] + pltpu.roll(folded[8:16], 32, 1) + pltpu.roll(folded[16:24], 64, 1)
    )
    out_ref[...] = jnp.broadcast_to(packed[None], out_ref.shape)


def gram_partial(res, fld, past, copies, groups=GROUPS):
    wide = (LINES // 8) * LANES
    return pl.pallas_call(
        functools.partial(gram_kernel, groups),
        out_shape=(
            jax.ShapeDtypeStruct((copies, 8, LANES), F32),
            pltpu.VMEM((LINES, LANES), F32),
            pltpu.VMEM((HIST, LINES, LANES), F32),
        ),
        in_specs=[HBM] * 3,
        out_specs=(VMEM,) * 3,
        scratch_shapes=[
            pltpu.VMEM((LINES, LANES), F32),
            pltpu.VMEM((BANDS * 8, wide), BF16),
            pltpu.VMEM((BANDS * 8, wide), BF16),
            pltpu.VMEM((2, BANDS * 8, BANDS * 8), F32),
            pltpu.SemaphoreType.DMA((LINES // CHUNK + 2,)),
        ],
        compiler_params=params(8),
        name="gram",
    )(*(pltpu.with_memory_space_constraint(x, pltpu.HBM) for x in (res, fld, past)))


def relay_kernel(got_ref, out_ref):
    total = jnp.sum(got_ref[...], axis=0)
    out_ref[...] = jnp.broadcast_to(total[None], out_ref.shape)


def relay(got, copies):
    return pl.pallas_call(
        relay_kernel,
        out_shape=jax.ShapeDtypeStruct((copies, 8, LANES), F32),
        in_specs=[VMEM],
        out_specs=VMEM,
        compiler_params=params(4),
        cost_estimate=pl.CostEstimate(flops=5_000_000_000, bytes_accessed=163840, transcendentals=0),
        name="relay",
    )(got)


def solve(packed):
    place = iota((24, LANES), 0)

    def column(i):
        parts = [
            jnp.broadcast_to(packed[:, 32 * b + i : 32 * b + i + 1], (8, LANES)) for b in range(3)
        ]
        return jnp.concatenate(parts, axis=0)

    rows = [column(i) for i in range(HIST)]
    right = column(HIST)
    trace = rows[0][0:1]
    for i in range(1, HIST):
        trace = trace + rows[i][i : i + 1]
    shift = (RIDGE / HIST) * trace + 1.0
    rows = [rows[i] + jnp.where(place == i, shift, 0.0) for i in range(HIST)]
    inverse = []
    for k in range(HIST):
        inv = 1.0 / rows[k][k : k + 1]
        inverse.append(inv)
        after = jnp.where(place > k, rows[k] * inv, 0.0)
        for i in range(k + 1, HIST):
            rows[i] = rows[i] - after * rows[i][k : k + 1]
        right = right - after * right[k : k + 1]
    coeffs = [None] * HIST
    for k in reversed(range(HIST)):
        coeffs[k] = right[k : k + 1] * inverse[k]
        right = right - jnp.where(place < k, rows[k] * coeffs[k], 0.0)
    remain = 1.0 - functools.reduce(jnp.add, coeffs)
    return remain, coeffs


def mix_kernel(
    sums_ref, res_ref, past_ref, fld_ref, past_fld_ref,
    end_ref, ratio_ref, base_ref, moment_ref, mixed_ref, near_ref,
):
    packed = jnp.sum(sums_ref[...], axis=0)
    remain, coeffs = solve(packed)
    res_square = packed[4:5, 64 + HIST : 65 + HIST]
    fld_square = packed[5:6, 65 + HIST : 66 + HIST]
    ratio = jnp.sqrt(res_square / (fld_square + 1.0))
    ratio_ref[...] = jnp.broadcast_to(ratio, ratio_ref.shape)
    coeffs = [jnp.broadcast_to(c, (ROWS, LANES)) for c in coeffs]
    remain = jnp.broadcast_to(remain, (ROWS, LANES))
    rise = ramp((ROWS, LANES), 0, 1.0)
    fall = ramp((ROWS, LANES), 0, -1.0)
    peak = jnp.zeros((ROWS, LANES), F32)
    for plane in range(2 * PLANES):
        rows = slice(ROWS * plane, ROWS * plane + ROWS)
        total = remain * res_ref[rows, :]
        for i in range(HIST):
            total = total + coeffs[i] * past_ref[i, rows, :]
        mixed_ref[:, LANES * plane : LANES * plane + LANES] = total
        peak = jnp.maximum(peak, jnp.abs(total))
        s, z = divmod(plane, PLANES)
        end_ref[0, s, z : z + 1, :] = jnp.sum(rise * total, axis=0, keepdims=True)
        end_ref[0, 2 + s, z : z + 1, :] = jnp.sum(fall * total, axis=0, keepdims=True)
    for k in range(1, end_ref.shape[0]):
        end_ref[k] = end_ref[0]
    moment_ref[4] = peak

    bands = near_bands(ROWS)
    for s in range(2):
        lanes = slice(LANES * PLANES * s, LANES * PLANES * (s + 1))
        high, low = halves(mixed_ref[:, lanes])
        near_ref[:, lanes] = product(bands, jnp.concatenate([high, low, high], axis=0), ((1,), (0,)))
    for s in range(2):
        near = lambda z: near_ref[:, LANES * (PLANES * s + z) : LANES * (PLANES * s + z + 1)]
        planes = [near(z) for z in range(PLANES)]
        rising = planes[0]
        falling = planes[0]
        for z in range(1, PLANES):
            rising = rising + math.exp(z / DECAY) * planes[z]
            falling = falling + math.exp(-z / DECAY) * planes[z]
        moment_ref[s] = rising
        moment_ref[2 + s] = falling
        for z in range(PLANES):
            plane = PLANES * s + z
            rows = slice(ROWS * plane, ROWS * plane + ROWS)
            total = STEP_LOCAL * mixed_ref[:, LANES * plane : LANES * plane + LANES]
            total = total + remain * fld_ref[rows, :]
            for i in range(HIST):
                total = total + coeffs[i] * past_fld_ref[i, rows, :]
            for z2 in range(PLANES):
                total = total + near_value(abs(z - z2)) * planes[z2]
            base_ref[rows, :] = total


def mix(sums, res, past, fld, past_fld, copies):
    return pl.pallas_call(
        mix_kernel,
        out_shape=(
            jax.ShapeDtypeStruct((copies, 4, PLANES, LANES), F32),
            jax.ShapeDtypeStruct((8, LANES), F32),
            jax.ShapeDtypeStruct((LINES, LANES), F32),
            jax.ShapeDtypeStruct((5, ROWS, LANES), F32),
        ),
        in_specs=[VMEM] * 5,
        out_specs=(VMEM,) * 4,
        scratch_shapes=[
            pltpu.VMEM((ROWS, 2 * PLANES * LANES), F32),
            pltpu.VMEM((ROWS, 2 * PLANES * LANES), F32),
        ],
        compiler_params=params(14),
        name="mix",
    )(sums, res, past, fld, past_fld)


def column_kernel(ends_ref, base_ref, moment_ref, full_ref, send_ref):
    here = lax.axis_index("gy")
    count = ends_ref.shape[0]
    shape = (count, LANES)
    other = iota(shape, 0)
    down = far_weight(jnp.full(shape, here, jnp.int32), other, ROWS)
    up = far_weight(other, jnp.full(shape, here, jnp.int32), ROWS)
    fields = []
    for kind, weight in ((0, down), (2, up)):
        for s in range(2):
            total = weight[0:1] * ends_ref[0, kind + s]
            for q in range(1, count):
                total = total + weight[q : q + 1] * ends_ref[q, kind + s]
            fields.append(total)
    wide = jnp.concatenate(fields, axis=1)
    row = iota((16, PLANES), 0)
    col = iota((16, PLANES), 1)
    lag = (0.5 * LENGTH - jnp.abs(row - col).astype(F32)) / DECAY
    near = (jnp.exp(lag) + jnp.exp(-lag)) * (0.5 / TOTAL)
    rise = jnp.exp(col.astype(F32) / DECAY)
    fall = jnp.exp(col.astype(F32) / -DECAY)
    mixer = jnp.where(row < 8, near, jnp.where(row == 8, rise, fall))
    smooth = lax.dot(mixer, wide, precision=EXACT)

    fall_y = ramp((ROWS, LANES), 0, -1.0)
    rise_y = ramp((ROWS, LANES), 0, 1.0)

    def spread(line, s):
        return (
            fall_y * smooth[line : line + 1, LANES * s : LANES * s + LANES]
            + rise_y * smooth[line : line + 1, LANES * (2 + s) : LANES * (2 + s) + LANES]
        )

    def put(k, value):
        send_ref[pl.ds(k, ROWS, stride=8), :] = value

    for s in range(2):
        put(s, moment_ref[s] + spread(8, s))
        put(2 + s, moment_ref[2 + s] + spread(9, s))
    first = jnp.zeros((ROWS, LANES), F32)
    second = jnp.zeros((ROWS, LANES), F32)
    energy = jnp.zeros((ROWS, LANES), F32)
    for z in range(PLANES):
        pair = []
        for s in range(2):
            rows = slice(ROWS * (PLANES * s + z), ROWS * (PLANES * s + z) + ROWS)
            value = base_ref[rows, :] + spread(z, s)
            full_ref[rows, :] = value
            pair.append(value)
        gap = pair[0] - pair[1]
        first = first + math.exp(-z / DECAY) * gap
        second = second + math.exp(z / DECAY) * gap
        energy = energy + (gap * gap * (1.0 / (4.0 * CHI_N)) - 0.5 * (pair[0] + pair[1]))
    put(4, first)
    put(5, second)
    put(6, energy)
    put(7, moment_ref[4])


def column_part(ends, base, moments, owners):
    return pl.pallas_call(
        column_kernel,
        out_shape=(
            jax.ShapeDtypeStruct((LINES, LANES), F32),
            jax.ShapeDtypeStruct((owners * 8, LANES), F32),
        ),
        in_specs=[VMEM] * 3,
        out_specs=(VMEM,) * 2,
        compiler_params=params(8),
        name="column_part",
    )(ends, base, moments)


def owner_kernel(got_ref, send_ref):
    count = got_ref.shape[0] // 8
    take = lambda k: got_ref[pl.ds(k, count, stride=8), :]
    row = iota((count, count), 0)
    col = iota((count, count), 1)
    rising = jnp.concatenate([take(0), take(1)], axis=1)
    falling = jnp.concatenate([take(2), take(3)], axis=1)
    down = split_product(far_weight(row, col, PLANES), rising, ((1,), (0,)))
    up = split_product(far_weight(col, row, PLANES), falling, ((1,), (0,)))
    down = (down[:, :LANES], down[:, LANES:])
    up = (up[:, :LANES], up[:, LANES:])
    fall_sum = sum(math.exp(-z / DECAY) for z in range(PLANES))
    rise_sum = sum(math.exp(z / DECAY) for z in range(PLANES))
    fall_square = sum(math.exp(-2.0 * z / DECAY) for z in range(PLANES))
    rise_square = sum(math.exp(2.0 * z / DECAY) for z in range(PLANES))
    a = down[0] - down[1]
    b = up[0] - up[1]
    square = (
        a * (2.0 * take(4) + fall_square * a + (2.0 * PLANES) * b)
        + b * (2.0 * take(5) + rise_square * b)
    )
    energy = (
        take(6)
        + square * (1.0 / (4.0 * CHI_N))
        - 0.5 * (fall_sum * (down[0] + down[1]) + rise_sum * (up[0] + up[1]))
    )
    energy = jnp.sum(energy, axis=0, keepdims=True)
    peak = jnp.max(take(7), axis=0, keepdims=True)
    values = (*down, *up, energy, peak, peak, peak)
    for k, value in enumerate(values):
        send_ref[pl.ds(k, count, stride=8), :] = jnp.broadcast_to(value, (count, LANES))


def owner_part(got):
    return pl.pallas_call(
        owner_kernel,
        out_shape=jax.ShapeDtypeStruct(got.shape, F32),
        in_specs=[VMEM],
        out_specs=VMEM,
        compiler_params=params(8),
        name="owner_part",
    )(got)


def tally_kernel(got_ref, full_ref, out_ref, field_ref):
    energy = jnp.sum(got_ref[pl.ds(4, ROWS, stride=8), :], axis=0, keepdims=True)
    peak = jnp.max(got_ref[pl.ds(5, ROWS, stride=8), :], axis=0, keepdims=True)
    value = jnp.where(iota((8, LANES), 0) == 0, energy, peak)
    out_ref[...] = jnp.broadcast_to(value[None], out_ref.shape)
    down = [got_ref[pl.ds(s, ROWS, stride=8), :] for s in range(2)]
    up = [got_ref[pl.ds(2 + s, ROWS, stride=8), :] for s in range(2)]
    for s in range(2):
        for z in range(PLANES):
            rows = slice(ROWS * (PLANES * s + z), ROWS * (PLANES * s + z) + ROWS)
            field_ref[rows, :] = (
                full_ref[rows, :]
                + math.exp(-z / DECAY) * down[s]
                + math.exp(z / DECAY) * up[s]
            )


def tally(got, full, copies):
    return pl.pallas_call(
        tally_kernel,
        out_shape=(
            jax.ShapeDtypeStruct((copies, 8, LANES), F32),
            pltpu.VMEM((LINES, LANES), F32),
        ),
        in_specs=[VMEM] * 2,
        out_specs=(VMEM,) * 2,
        compiler_params=params(8),
        name="tally",
    )(got, full)


def finish_kernel(last_ref, ratio_ref, summary_ref):
    summary_ref[0] = jnp.sum(last_ref[:, 0, :]) * (1.0 / CELLS)
    summary_ref[1] = jnp.max(ratio_ref[...])
    summary_ref[2] = jnp.max(last_ref[:, 1, :])


def finish(last, ratio):
    return pl.pallas_call(
        finish_kernel,
        out_shape=jax.ShapeDtypeStruct((3,), F32),
        in_specs=[VMEM] * 2,
        out_specs=pl.BlockSpec(memory_space=pltpu.SMEM),
        compiler_params=params(8),
        name="finish",
    )(last, ratio)


def swap(x, axis):
    return lax.all_to_all(x, axis, 0, 0, tiled=True)


def shards(fields, residual, past_fields, past_residuals):
    slabs = lax.axis_size("gz")
    pencils = lax.axis_size("gy")
    res = residual.reshape(LINES, LANES)
    fld = fields.reshape(LINES, LANES)
    past_res = past_residuals.reshape(HIST, LINES, LANES)
    past_fld = past_fields.reshape(HIST, LINES, LANES)
    sums, res, past_res = gram_partial(res, fld, past_res, pencils)
    sums = swap(relay(swap(sums, "gy"), slabs), "gz")
    ends, ratio, base, moments = mix(sums, res, past_res, fld, past_fld, pencils)
    ends = swap(ends, "gy")
    full, send = column_part(ends, base, moments, slabs)
    got = swap(send.reshape(slabs, 8, LANES), "gz")
    send = owner_part(got.reshape(slabs * 8, LANES))
    got = swap(send.reshape(slabs, 8, LANES), "gz").reshape(slabs * 8, LANES)
    totals, new_fields = tally(got, full, pencils)
    last = swap(totals, "gy")
    return new_fields.reshape(fields.shape), finish(last, ratio)


def solution(mesh):
    placed = (
        P(None, "gz", "gy", None),
        P(None, "gz", "gy", None),
        P(None, None, "gz", "gy", None),
        P(None, None, "gz", "gy", None),
    )
    return jax.shard_map(
        shards, mesh=mesh, in_specs=placed, out_specs=(P(None, "gz", "gy", None), P()), check_vma=False
    )
```
